32 devices in a mesh: gx: 4 (over z), gy: 2 (over y), gz: 4 (over x, core).
Axes of the slice: x: 2, y: 2, z: 4, core: 2. Of those that a mesh axis runs over, the one named last changes fastest.
Arguments:
- start_disp: float32 [3, 32, 16, 512], P(None, 'gx', 'gy', 'gz'), may hold values from -2 to 2
- inertial: float32 [3, 32, 16, 512], P(None, 'gx', 'gy', 'gz'), may hold values from -1 to 1
- material: int32 [32, 16, 512], P('gx', 'gy', 'gz'), may hold values from 0 to 7
- pinned: int32 [32, 16, 512], P('gx', 'gy', 'gz'), may hold values 0 or 1
- stiffness: float32 [8], replicated, may hold values from 3 to 100
Outputs:
- displacement: float32 [3, 32, 16, 512], P(None, 'gx', 'gy', 'gz')
The draws below stay inside these ranges and needn't reach their ends.
All inputs are finite; a program needn't handle non-finite values. No bound on the sum of `pinned` on one device may be relied on, other than what follows from the above.
Results may differ from the reference program's by a relative error of at most 0.0003.
Values sent between devices are 32-bit elements; how exact they have to be, the bound alone decides.
A program may use at most 64 MiB of HBM per device.

```python
import math
import jax
import jax.numpy as jnp
from jax import lax

CX = 8
ITERS = 4
POLAR_STEPS = 6
MATS = 8
NX = 32
NY = 16
NZ = 512


def set_ends(drawn, rng, low, largest):
    spot = [jax.random.randint(jax.random.fold_in(rng, axis), (), 0, length) for axis, length in enumerate(drawn.shape)]
    main_axis = drawn.shape.index(max(drawn.shape))
    next_to = spot[:main_axis] + [(spot[main_axis] + 1) % drawn.shape[main_axis]] + spot[main_axis + 1:]
    return drawn.at[tuple(spot)].set(low).at[tuple(next_to)].set(largest)


def levels(own_key, dims, split, low, largest):
    loudness, own = 1.0, jax.random.fold_in(own_key, 6)
    for position, shards_of in split:
        draws = jnp.exp(jax.random.uniform(jax.random.fold_in(own, position), (shards_of,), jnp.float32, low / len(split), largest / len(split)))
        loudness = loudness * jnp.repeat(draws, dims[position] // shards_of).reshape([-1 if axis == position else 1 for axis in range(len(dims))])
    return loudness


def gaussian(stream_key, extent, spread, most, cuts=(), kind=jnp.bfloat16):
    level = levels(stream_key, extent, cuts, -0.22, 0.18) if cuts else 1.0
    values = jax.random.normal(stream_key, extent, jnp.float32) * spread * level
    return jnp.minimum(jnp.maximum(values, -most), most).astype(kind)


def setup_inputs(seed: int = 0) -> dict:
    key_of = jax.random.split(jax.random.key(seed), 6)
    return {
        "start_disp": gaussian(key_of[0], (3, NX, NY, NZ), 0.5, 2.0, ((1, 4), (2, 2), (3, 4)), jnp.float32),
        "inertial": gaussian(key_of[1], (3, NX, NY, NZ), 0.25, 1.0, ((1, 4), (2, 2), (3, 4)), jnp.float32),
        "material": set_ends(jax.random.randint(key_of[2], (NX, NY, NZ), 0, MATS), jax.random.fold_in(key_of[2], 1), 0, MATS - 1).astype(jnp.int32),
        "pinned": set_ends((jax.random.randint(key_of[3], (NX, NY, NZ), 0, 16) < 1).astype(jnp.int32), jax.random.fold_in(key_of[3], 1), 0, 1),
        "stiffness": jnp.clip(jnp.exp(jax.random.uniform(key_of[4], (MATS,), jnp.float32, math.log(3.0), math.log(100.0))), 3.0, 100.0),
    }


inertia = 1.0
relax = 0.6
radius = 0.9

def forward_diff(field, axis):
    size = field.shape[axis]
    return lax.slice_in_dim(field, 1, size, axis=axis) - lax.slice_in_dim(field, 0, size - 1, axis=axis)

def pair_sum(field, axis):
    size = field.shape[axis]
    return lax.slice_in_dim(field, 1, size, axis=axis) + lax.slice_in_dim(field, 0, size - 1, axis=axis)

def gradient(field, axis):
    result = forward_diff(field, axis)
    for other in range(3):
        if other != axis:
            result = pair_sum(result, other)
    return 0.25 * result

def project(nodes, welem):
    deform = [[gradient(nodes[c], d) + (1.0 if c == d else 0.0) for d in range(3)] for c in range(3)]
    total = sum((deform[c][d] * deform[c][d] for c in range(3) for d in range(3)))
    scale = jnp.maximum(jnp.sqrt(total / 3.0), 1.0)
    rotate = [[deform[c][d] / scale for d in range(3)] for c in range(3)]
    for step in range(POLAR_STEPS):
        middle = [[(1.5 if i == j else 0.0) - 0.5 * sum((rotate[k][i] * rotate[k][j] for k in range(3))) for j in range(3)] for i in range(3)]
        rotate = [[sum((rotate[c][j] * middle[j][d] for j in range(3))) for d in range(3)] for c in range(3)]
    return [welem * (deform[c][d] - rotate[c][d]) for c in range(3) for d in range(3)]

def assemble(stress):
    forces = []
    for c in range(3):
        total = 0.0
        for d in range(3):
            term = stress[3 * c + d]
            for other in range(3):
                if other != d:
                    term = pair_sum(term, other)
            total = total - 0.25 * forward_diff(term, d)
        forces.append(total)
    return jnp.stack(forces)

def diagonal(welem):
    total = welem
    for axis in range(3):
        total = pair_sum(total, axis)
    return inertia + 3.0 / 16.0 * total

def lookup(material, stiffness):
    total = jnp.zeros(material.shape, jnp.float32)
    for index in range(MATS):
        total = total + jnp.where(material == index, stiffness[index], 0.0)
    return total

def reference(start_disp, inertial, material, pinned, stiffness):
    grid_x = lax.broadcasted_iota(jnp.int32, material.shape, 0)
    grid_y = lax.broadcasted_iota(jnp.int32, material.shape, 1)
    grid_z = lax.broadcasted_iota(jnp.int32, material.shape, 2)
    valid = (grid_x < NX - 1) & (grid_y < NY - 1) & (grid_z < NZ - 1)
    weights = jnp.where(valid, lookup(material, stiffness), 0.0)
    welem = jnp.pad(weights, ((1, 0), (1, 0), (1, 0)))
    diag = diagonal(welem)
    pins = pinned[None] > 0
    disp = jnp.where(pins, inertial, start_disp)
    previous = disp
    omega = 1.0
    blocks = NX // CX
    for step in range(ITERS):
        padded = jnp.pad(disp, ((0, 0), (1, 1), (1, 1), (1, 1)))

        def block_forces(index):
            start = (index * CX).astype(jnp.int32)
            nodes = lax.dynamic_slice_in_dim(padded, start, CX + 2, 1)
            wslab = lax.dynamic_slice_in_dim(welem, start, CX + 1, 0)
            return assemble(project([nodes[0], nodes[1], nodes[2]], wslab))
        parts = lax.map(block_forces, jnp.arange(blocks, dtype=jnp.int32))
        forces = jnp.moveaxis(parts, 0, 1).reshape(3, NX, NY, NZ)
        target = disp - relax * (inertia * (disp - inertial) + forces) / diag[None]
        if step == 0:
            fresh = target
        else:
            omega = 2.0 / (2.0 - radius * radius) if step == 1 else 4.0 / (4.0 - radius * radius * omega)
            fresh = omega * (target - previous) + previous
        fresh = jnp.where(pins, inertial, fresh)
        previous = disp
        disp = fresh
    return disp
```

```python
import functools

import jax
import jax.numpy as jnp
from jax import lax
from jax.experimental import pallas as pl
from jax.experimental.pallas import tpu as pltpu
from jax.sharding import PartitionSpec as P

ITERS = 4
POLAR_STEPS = 6
MATS = 8

relax = 0.6
radius = 0.9
HALO = ITERS
SLOT = 2 * HALO
NARR = 8
GROUPS = 2
PAIRS = NARR // 2 // GROUPS
AXES = ("gx", "gy", "gz")


def loop(lo, hi, body, unroll=2):
    assert (hi - lo) % unroll == 0

    def group(k, _):
        body([lo + k * unroll + i for i in range(unroll)])
        return 0

    lax.fori_loop(0, (hi - lo) // unroll, group, 0)


def node_terms(u, uz, roll_y):
    zs, zd = uz + u, uz - u
    ys, yd = roll_y(zs), roll_y(zd)
    return zs + ys, ys - zs, zd + yd


def stretch(low, high):
    deform = []
    for c in range(3):
        dx = high[c][0] - low[c][0]
        dy = high[c][1] + low[c][1]
        dz = high[c][2] + low[c][2]
        row = [dx, dy, dz]
        row[c] = row[c] + 1.0
        deform.append(row)
    return deform


COSINE = (
    1.00000005, 1.15469445, -0.222086479, 0.105738212,
    -0.0606261262, 0.0323189784, -0.0123398994, 0.00230085802,
)


def stress(deform, w):
    f = deform
    s = {}
    for i in range(3):
        for j in range(i, 3):
            s[i, j] = f[0][i] * f[0][j] + f[1][i] * f[1][j] + f[2][i] * f[2][j]
    mean = (s[0, 0] + s[1, 1] + s[2, 2]) * (1.0 / 3.0)
    inv = jnp.minimum(lax.rsqrt(mean), 1.0)
    k11, k22, k33 = (s[i, i] - mean for i in range(3))
    k12, k13, k23 = s[0, 1], s[0, 2], s[1, 2]
    a11, a12, a13, a23 = k11 * k11, k12 * k12, k13 * k13, k23 * k23
    b23, c23 = k22 * k33, k12 * k13
    spread = a11 - b23 + a12 + (a13 + a23)
    spread = jnp.maximum(spread * (1.0 / 3.0), 1e-30)
    rp = lax.rsqrt(spread)
    rp2 = rp * rp
    det = k11 * (b23 - a23) - k22 * a13 + ((c23 + c23) * k23 - k33 * a12)
    half = 0.5 + 0.25 * (det * rp * rp2)
    half = jnp.minimum(jnp.maximum(half, 1e-12), 1.0)
    root = half * lax.rsqrt(half)
    e = COSINE[-1]
    for a in COSINE[-2::-1]:
        e = e * root + a
    t2 = jnp.maximum(3.0 - 0.75 * (e * e), 1e-12)
    y = lax.rsqrt(t2)
    t = t2 * y
    e2 = 0.5 * e
    e3 = e + e2
    x2, x3 = t - e2, t + e2
    r12 = 1.0 / jnp.maximum(e3 - t, 1e-6)
    r13 = 1.0 / (e3 + t)
    r23 = 0.5 * y
    scale = 0.5 * (inv * inv)
    p = spread * rp * scale
    mean = mean * scale
    inv = inv * w
    qs = []
    for h in (mean + p * e, mean + p * x2, mean - p * x3):
        m = 1.5 - h
        q = inv * m
        for _ in range(POLAR_STEPS - 1):
            h = h * (m * m)
            m = 1.5 - h
            q = q * m
        qs.append(q)
    q12 = (qs[0] - qs[1]) * r12
    q23 = (qs[1] - qs[2]) * r23
    c2 = (q12 - q23) * r13
    c0 = (w - qs[0]) + (q12 * e - c2 * (e * x2))
    c1 = (c2 * x3 - q12) * rp
    c2 = c2 * rp2
    g = {
        (0, 0): (c0 + c1 * k11) - c2 * (a11 + (a12 + a13)),
        (1, 1): (c0 + c1 * k22) - c2 * (k22 * k22 + (a12 + a23)),
        (2, 2): (c0 + c1 * k33) - c2 * (k33 * k33 + (a13 + a23)),
        (0, 1): c1 * k12 - c2 * (k13 * k23 - k12 * k33),
        (0, 2): c1 * k13 - c2 * (k12 * k23 - k13 * k22),
        (1, 2): c1 * k23 - c2 * (c23 - k23 * k11),
    }
    pick = lambda i, j: g[min(i, j), max(i, j)]
    return [
        f[c][0] * pick(0, d) + f[c][1] * pick(1, d) + f[c][2] * pick(2, d)
        for c in range(3) for d in range(3)
    ]


def node_sums(before, here, roll_y):
    a = before[0] - here[0]
    b = before[1] + here[1]
    e = before[2] + here[2]
    g = (a - b) + roll_y(a + b)
    e = e + roll_y(e)
    return g - e, g + e


def advance(u, prev, inert, pin, rate, f, omega):
    target = u - rate * ((u - inert) + f)
    fresh = target if omega is None else omega * (target - prev) + prev
    return jnp.where(pin > 0.0, inert, fresh)


def kernel(
    counts, start, inertial, material, pinned, stiff, out,
    xe, sy, ry, ext, az, rz, prev, rate, terms, press, strip, sprev, srate, hz,
    send_sem, recv_sem,
):
    size_x, size_y, size_z = material.shape
    here = [lax.axis_index(a) for a in AXES]
    has = [[here[i] > 0, here[i] < counts[i] - 1] for i in range(3)]

    sub = lax.broadcasted_iota(jnp.int32, (size_y, size_z), 0)
    lane = lax.broadcasted_iota(jnp.int32, (size_y, size_z), 1)
    inside = ((sub < size_y - 1) | has[1][1]) & ((lane < size_z - 1) | has[2][1])
    quarter = [stiff[i] * 0.25 for i in range(MATS)]

    barrier = pltpu.get_barrier_semaphore()

    def peer(i, side):
        return {AXES[i]: here[i] + (1 if side else -1)}

    for i in range(3):
        for side in range(2):
            @pl.when(has[i][side])
            def _(i=i, side=side):
                pl.semaphore_signal(
                    barrier, inc=1, device_id=peer(i, side), device_id_type=pl.DeviceIdType.MESH
                )

    def faces(first, second):
        low = jnp.where(sub < HALO, first, pltpu.roll(second, HALO, 0))
        high = jnp.where(sub < HALO, pltpu.roll(first, HALO, 0), second)
        return low, high

    def pack_y(group, xs):
        done = [
            (p, x, faces(xe[2 * p, x], xe[2 * p + 1, x]))
            for x in xs for p in range(group * PAIRS, (group + 1) * PAIRS)
        ]
        for p, x, (low, high) in done:
            sy[0, p, x] = low
            sy[1, p, x] = high

    def own_planes(xs):
        done = []
        for x in xs:
            mat = material[x]
            w = jnp.zeros((size_y, size_z), jnp.float32)
            for index in range(MATS):
                w = jnp.where(mat == index, quarter[index], w)
            keep = inside & ((x < size_x - 1) | has[0][1])
            pins = pinned[x] > 0
            inert = [inertial[c, x] for c in range(3)]
            arrays = [jnp.where(pins, inert[c], start[c, x]) for c in range(3)] + inert
            arrays += [jnp.where(keep, w, 0.0), jnp.where(pins, 1.0, 0.0)]
            done.append((x + HALO, arrays))
        for x, arrays in done:
            for a in range(NARR):
                xe[a, x] = arrays[a]
            for p in range(NARR // 2):
                low, high = faces(arrays[2 * p], arrays[2 * p + 1])
                sy[0, p, x] = low
                sy[1, p, x] = high

    loop(0, size_x, own_planes, 4)

    def zero(ref, lo, n):
        def body(x, _):
            for a in range(ref.shape[0]):
                ref[a, x] = jnp.zeros(ref.shape[2:], jnp.float32)
            return 0
        lax.fori_loop(lo, lo + n, body, 0)

    top = HALO + size_x
    for side, lo in ((0, 0), (1, top)):
        @pl.when(jnp.logical_not(has[0][side]))
        def _(lo=lo):
            zero(xe, lo, HALO)
            for row in range(2):
                zero(ry.at[row, pl.ds(PAIRS, PAIRS)], lo, HALO)
    for side in range(2):
        @pl.when(jnp.logical_not(has[1][side]))
        def _(side=side):
            zero(ry.at[side], 0, top + HALO)

    n = 0
    for i in range(3):
        for side in range(2):
            n = n + has[i][side].astype(jnp.int32)
    pl.semaphore_wait(barrier, n)

    def remote(src, dst, k, i, side):
        return pltpu.make_async_remote_copy(
            src_ref=src, dst_ref=dst, send_sem=send_sem.at[k], recv_sem=recv_sem.at[k],
            device_id=peer(i, side), device_id_type=pl.DeviceIdType.MESH,
        )

    def x_copy(side, group):
        span = pl.ds(2 * PAIRS * group, 2 * PAIRS)
        src = xe.at[span, pl.ds(HALO if side == 0 else size_x, HALO)]
        dst = xe.at[span, pl.ds(top if side == 0 else 0, HALO)]
        return remote(src, dst, 2 * group + side, 0, side)

    def y_copy(side, part, group):
        lo, count = ((0, HALO), (HALO, size_x), (top, HALO))[part]
        span = pl.ds(PAIRS * group, PAIRS)
        return remote(
            sy.at[side, span, pl.ds(lo, count)], ry.at[1 - side, span, pl.ds(lo, count)],
            2 * GROUPS + (2 * part + side) * GROUPS + group, 1, side,
        )

    def corner(row, side):
        span = pl.ds(PAIRS, PAIRS)
        return remote(
            ry.at[row, span, pl.ds(HALO if side == 0 else size_x, HALO)],
            ry.at[row, span, pl.ds(top if side == 0 else 0, HALO)],
            8 * GROUPS + 2 + 2 * row + side, 0, side,
        )

    def z_copy(side):
        return remote(az, rz.at[1 - side], 8 * GROUPS + side, 2, side)

    def each(i, action):
        for side in range(2):
            @pl.when(has[i][side])
            def _(side=side):
                action(side)

    for group in range(GROUPS):
        each(0, lambda side: x_copy(side, group).start())
        each(1, lambda side: y_copy(side, 1, group).start())
    each(0, lambda side: x_copy(1 - side, 0).wait_recv())
    loop(0, HALO, functools.partial(pack_y, 0), HALO)
    loop(top, top + HALO, functools.partial(pack_y, 0), HALO)
    for part in (0, 2):
        each(1, lambda side: y_copy(side, part, 0).start())
    each(1, lambda row: y_copy(1 - row, 1, 1).wait_recv())
    each(1, lambda row: each(0, lambda side: corner(row, side).start()))

    wide = lax.broadcasted_iota(jnp.int32, (2 * HALO + size_y, size_z), 1)

    def fill(xs):
        done = []
        for x in xs:
            for p in range(NARR // 2):
                lo, hi = ry[0, p, x], ry[1, p, x]
                for q in range(2):
                    a = 2 * p + q
                    own = pltpu.roll(xe[a, x], HALO, 0)
                    lo_part = lo if q == 0 else pltpu.roll(lo, HALO, 0)
                    hi_part = hi if q == 1 else pltpu.roll(hi, HALO, 0)
                    done.append((
                        a, x, jnp.where(sub < HALO, lo_part, own),
                        jnp.where(sub < HALO, own, hi_part),
                    ))
        for a, x, low, high in done:
            ext[a, x, 0:size_y] = low
            ext[a, x, size_y : 2 * size_y] = high

    each(1, lambda row: y_copy(1 - row, 1, 0).wait_recv())
    loop(HALO, top, fill, 4)
    each(0, lambda side: x_copy(1 - side, 1).wait_recv())
    for part in (0, 2):
        each(1, lambda row: y_copy(1 - row, part, 0).wait_recv())
    each(1, lambda row: each(0, lambda side: corner(row, 1 - side).wait_recv()))
    loop(0, HALO, fill, HALO)
    loop(top, top + HALO, fill, HALO)

    planes = top + HALO

    def pack_z(arrays):
        packed = [jnp.zeros(wide.shape, jnp.float32) for _ in arrays]
        for x in range(planes):
            spot = (wide >= x * SLOT) & (wide < (x + 1) * SLOT)
            for k, a in enumerate(arrays):
                moved = pltpu.roll(ext[a, x], (x * SLOT + HALO) % size_z, 1)
                packed[k] = jnp.where(spot, moved, packed[k])
        for a, value in zip(arrays, packed):
            az[a] = value

    loop(0, NARR, pack_z, 4)
    each(2, lambda side: z_copy(side).start())

    rows = 2 * HALO + size_y
    up = lambda v: pltpu.roll(v, rows - 1, 0)
    down = lambda v: pltpu.roll(v, 1, 0)
    zup = lambda v: pltpu.roll(v, size_z - 1, 1)
    zdown = lambda v: pltpu.roll(v, 1, 1)

    def begin(xs):
        us = [(x, c, ext[c, x]) for x in xs for c in range(3)]
        for x, c, u in us:
            prev[c, x] = u

    def weigh(xs):
        sums = [ext[6, x - 1] + ext[6, x] for x in xs]
        sums = [w + down(w) for w in sums]
        for x, w in zip(xs, sums):
            rate[x] = w

    loop(0, planes, begin, 4)
    loop(1, planes - 1, weigh, (planes - 2) // 2)
    for side in range(2):
        @pl.when(jnp.logical_not(has[2][side]))
        def _(side=side):
            for a in range(NARR):
                rz[side, a] = jnp.zeros(wide.shape, jnp.float32)
    each(2, lambda side: z_copy(1 - side).wait_recv())

    early = lax.rem(wide, SLOT) < HALO
    for a in range(NARR):
        strip[0, a] = jnp.where(early, rz[0, a], az[a])
        strip[1, a] = jnp.where(early, az[a], rz[1, a])

    xup = lambda v: pltpu.roll(v, size_z - SLOT, 1)
    xdown = lambda v: pltpu.roll(v, SLOT, 1)

    def speed(total):
        return relax / (1.0 + 0.75 * total)

    for s in range(2):
        w = strip[s, 6]
        w = w + xdown(w)
        w = w + down(w)
        if s == 0:
            hz[0] = w
        srate[s] = speed(w + zdown(w))
        for c in range(3):
            sprev[s, c] = strip[s, c]

    first_lane = wide == 0
    last_lane = wide == size_z - 1

    def from_low(v, x):
        return pltpu.roll(v, size_z - HALO + 1 - SLOT * x, 1)

    def from_high(v, x):
        return pltpu.roll(v, size_z - 1 - HALO - SLOT * x, 1)

    def make_terms(x, c, u):
        uz = jnp.where(last_lane, from_high(strip[1, c], x), zup(u))
        return node_terms(u * 0.25, uz * 0.25, up)

    def put_terms(done):
        for x, c, three in done:
            for k in range(3):
                terms[x, 3 * c + k] = three[k]

    def setup(xs):
        us = [(x, c, ext[c, x]) for x in xs for c in range(3)]
        done = [(x, c, make_terms(x, c, u)) for x, c, u in us]
        put_terms(done)

    def setup_rate(xs):
        done = []
        for x in xs:
            w = rate[x]
            done.append(speed(w + jnp.where(first_lane, from_low(hz[0], x), zdown(w))))
        for x, r in zip(xs, done):
            rate[x] = r

    loop(0, planes, setup, 4)
    loop(1, planes - 1, setup_rate, (planes - 2) // 2)

    omega = None
    for step in range(ITERS):
        if step == 1:
            omega = 2.0 / (2.0 - radius * radius)
        elif step > 1:
            omega = 4.0 / (4.0 - radius * radius * omega)
        last = step == ITERS - 1

        def strips():
            done = []
            for s in range(2):
                low, high = [], []
                for c in range(3):
                    u = strip[s, c] * 0.25
                    t = node_terms(u, zup(u), up)
                    low.append(t)
                    high.append([xup(v) for v in t])
                p = stress(stretch(low, high), strip[s, 6])
                for c in range(3):
                    mine = p[3 * c : 3 * c + 3]
                    minus, plus = node_sums([xdown(v) for v in mine], mine, down)
                    u = strip[s, c]
                    fresh = advance(
                        u, sprev[s, c], strip[s, 3 + c], strip[s, 7], srate[s],
                        minus + zdown(plus), omega,
                    )
                    done.append((s, c, u, plus, fresh))
            for s, c, u, plus, fresh in done:
                if s == 0:
                    hz[c] = plus
                if not last:
                    sprev[s, c] = u
                    strip[s, c] = fresh

        def voxels(x, _):
            low = [[terms[x, 3 * c + k] for k in range(3)] for c in range(3)]
            high = [[terms[x + 1, 3 * c + k] for k in range(3)] for c in range(3)]
            p = stress(stretch(low, high), ext[6, x])
            for k in range(9):
                press[x, k] = p[k]
            return 0

        def nodes(xs):
            done = []
            for x in xs:
                for c in range(3):
                    minus, plus = node_sums(
                        [press[x - 1, 3 * c + k] for k in range(3)],
                        [press[x, 3 * c + k] for k in range(3)],
                        down,
                    )
                    f = minus + jnp.where(first_lane, from_low(hz[c], x), zdown(plus))
                    u = ext[c, x]
                    fresh = advance(u, prev[c, x], ext[3 + c, x], ext[7, x], rate[x], f, omega)
                    done.append((x, c, u, fresh))
            if last:
                for x, c, _, fresh in done:
                    out[c, x - HALO] = fresh[HALO : HALO + size_y]
                return
            later = [(x, c, make_terms(x, c, fresh)) for x, c, _, fresh in done]
            for x, c, u, fresh in done:
                prev[c, x] = u
                ext[c, x] = fresh
            put_terms(later)

        strips()
        lax.fori_loop(step, planes - 1 - step, voxels, 0)
        loop(step + 1, planes - 1 - step, nodes)

    for group in range(GROUPS):
        each(0, lambda side: x_copy(side, group).wait_send())
        each(1, lambda side: y_copy(side, 1, group).wait_send())
    for part in (0, 2):
        each(1, lambda side: y_copy(side, part, 0).wait_send())
    each(1, lambda row: each(0, lambda side: corner(row, side).wait_send()))
    each(2, lambda side: z_copy(side).wait_send())


def per_device(counts, start_disp, inertial, material, pinned, stiffness):
    size_x, size_y, size_z = material.shape
    planes, rows = size_x + 2 * HALO, size_y + 2 * HALO
    assert planes * SLOT == size_z and size_y == 2 * HALO
    vmem = pl.BlockSpec(memory_space=pltpu.VMEM)
    f32 = lambda *shape: pltpu.VMEM(shape, jnp.float32)
    return pl.pallas_call(
        functools.partial(kernel, counts),
        out_shape=jax.ShapeDtypeStruct(start_disp.shape, jnp.float32),
        in_specs=[vmem, vmem, vmem, vmem, pl.BlockSpec(memory_space=pltpu.SMEM)],
        out_specs=vmem,
        scratch_shapes=[
            f32(NARR, planes, size_y, size_z),
            f32(2, NARR // 2, planes, size_y, size_z),
            f32(2, NARR // 2, planes, size_y, size_z),
            f32(NARR, planes, rows, size_z),
            f32(NARR, rows, size_z),
            f32(2, NARR, rows, size_z),
            f32(3, planes, rows, size_z),
            f32(planes, rows, size_z),
            f32(planes, 9, rows, size_z),
            f32(planes, 9, rows, size_z),
            f32(2, NARR, rows, size_z),
            f32(2, 3, rows, size_z),
            f32(2, rows, size_z),
            f32(3, rows, size_z),
            pltpu.SemaphoreType.DMA((8 * GROUPS + 6,)),
            pltpu.SemaphoreType.DMA((8 * GROUPS + 6,)),
        ],
        compiler_params=pltpu.CompilerParams(collective_id=0, has_side_effects=True),
    )(start_disp, inertial, material, pinned, stiffness)


def solution(mesh):
    placed = (
        P(None, "gx", "gy", "gz"),
        P(None, "gx", "gy", "gz"),
        P("gx", "gy", "gz"),
        P("gx", "gy", "gz"),
        P(),
    )
    counts = tuple(mesh.shape[a] for a in AXES)
    return jax.shard_map(
        functools.partial(per_device, counts), mesh=mesh, in_specs=placed,
        out_specs=P(None, "gx", "gy", "gz"), check_vma=False,
    )
```

```python
import functools
import itertools

import jax
import jax.numpy as jnp
from jax import lax
from jax.experimental import pallas as pl
from jax.experimental.pallas import tpu as pltpu
from jax.sharding import PartitionSpec as P

ITERS = 4
POLAR_STEPS = 6
MATS = 8

relax = 0.6
radius = 0.9
HALO = ITERS
SLOT = 2 * HALO
NARR = 8
SPAN = NARR // 2
WEIGHT, INERT, PIN = 3, 4, 7
AXES = ("gx", "gy", "gz")
AROUND = tuple(o for o in itertools.product((-1, 0, 1), repeat=3) if any(o))
DIAGONAL = tuple(itertools.product((-1, 1), repeat=2))
FACES = len(AROUND)
CORNERS = FACES + 8
COPIES = CORNERS + 8


def loop(lo, hi, body, unroll=2):
    assert (hi - lo) % unroll == 0

    def group(k, _):
        body([lo + k * unroll + i for i in range(unroll)])
        return 0

    lax.fori_loop(0, (hi - lo) // unroll, group, 0)


def node_terms(u, uz, roll_y):
    zs, zd = uz + u, uz - u
    ys, yd = roll_y(zs), roll_y(zd)
    return zs + ys, ys - zs, zd + yd


def stretch(low, high):
    deform = []
    for c in range(3):
        dx = high[c][0] - low[c][0]
        dy = high[c][1] + low[c][1]
        dz = high[c][2] + low[c][2]
        row = [dx, dy, dz]
        row[c] = row[c] + 1.0
        deform.append(row)
    return deform


COSINE = (
    1.00000005, 1.15469445, -0.222086479, 0.105738212,
    -0.0606261262, 0.0323189784, -0.0123398994, 0.00230085802,
)


def stress(deform, w):
    f = deform
    s = {}
    for i in range(3):
        for j in range(i, 3):
            s[i, j] = f[0][i] * f[0][j] + f[1][i] * f[1][j] + f[2][i] * f[2][j]
    mean = (s[0, 0] + s[1, 1] + s[2, 2]) * (1.0 / 3.0)
    inv = jnp.minimum(lax.rsqrt(mean), 1.0)
    k11, k22, k33 = (s[i, i] - mean for i in range(3))
    k12, k13, k23 = s[0, 1], s[0, 2], s[1, 2]
    a11, a12, a13, a23 = k11 * k11, k12 * k12, k13 * k13, k23 * k23
    b23, c23 = k22 * k33, k12 * k13
    spread = a11 - b23 + a12 + (a13 + a23)
    spread = jnp.maximum(spread * (1.0 / 3.0), 1e-30)
    rp = lax.rsqrt(spread)
    rp2 = rp * rp
    det = k11 * (b23 - a23) - k22 * a13 + ((c23 + c23) * k23 - k33 * a12)
    half = 0.5 + 0.25 * (det * rp * rp2)
    half = jnp.minimum(jnp.maximum(half, 1e-12), 1.0)
    root = half * lax.rsqrt(half)
    e = COSINE[-1]
    for a in COSINE[-2::-1]:
        e = e * root + a
    t2 = jnp.maximum(3.0 - 0.75 * (e * e), 1e-12)
    y = lax.rsqrt(t2)
    t = t2 * y
    e2 = 0.5 * e
    e3 = e + e2
    x2, x3 = t - e2, t + e2
    r12 = 1.0 / jnp.maximum(e3 - t, 1e-6)
    r13 = 1.0 / (e3 + t)
    r23 = 0.5 * y
    scale = 0.5 * (inv * inv)
    p = spread * rp * scale
    mean = mean * scale
    inv = inv * w
    qs = []
    for h in (mean + p * e, mean + p * x2, mean - p * x3):
        m = 1.5 - h
        q = inv * m
        for _ in range(POLAR_STEPS - 1):
            h = h * (m * m)
            m = 1.5 - h
            q = q * m
        qs.append(q)
    q12 = (qs[0] - qs[1]) * r12
    q23 = (qs[1] - qs[2]) * r23
    c2 = (q12 - q23) * r13
    c0 = (w - qs[0]) + (q12 * e - c2 * (e * x2))
    c1 = (c2 * x3 - q12) * rp
    c2 = c2 * rp2
    g = {
        (0, 0): (c0 + c1 * k11) - c2 * (a11 + (a12 + a13)),
        (1, 1): (c0 + c1 * k22) - c2 * (k22 * k22 + (a12 + a23)),
        (2, 2): (c0 + c1 * k33) - c2 * (k33 * k33 + (a13 + a23)),
        (0, 1): c1 * k12 - c2 * (k13 * k23 - k12 * k33),
        (0, 2): c1 * k13 - c2 * (k12 * k23 - k13 * k22),
        (1, 2): c1 * k23 - c2 * (c23 - k23 * k11),
    }
    pick = lambda i, j: g[min(i, j), max(i, j)]
    return [
        f[c][0] * pick(0, d) + f[c][1] * pick(1, d) + f[c][2] * pick(2, d)
        for c in range(3) for d in range(3)
    ]


def node_sums(before, here, roll_y):
    a = before[0] - here[0]
    b = before[1] + here[1]
    e = before[2] + here[2]
    g = (a - b) + roll_y(a + b)
    e = e + roll_y(e)
    return g - e, g + e


def advance(u, prev, inert, rate, f, omega):
    target = u - rate * ((u - inert) + f)
    return target if omega is None else omega * (target - prev()) + prev()


def kernel(
    counts, start, inertial, material, pinned, stiff, out,
    first, mat, pins, ext, pk, rz, strip, sprev, srate, zin, prev, rate, terms, press, done,
    send_sem, recv_sem, load_sem,
):
    size_x, size_y, size_z = material.shape
    top = HALO + size_x
    planes = top + HALO
    rows = 2 * size_y
    own_y, own_x = pl.ds(0, size_y), pl.ds(HALO, size_x)
    here = [lax.axis_index(a) for a in AXES]
    has = [{-1: here[i] > 0, 1: here[i] < counts[i] - 1} for i in range(3)]

    loads = [
        pltpu.make_async_copy(pinned, pins, load_sem.at[0]),
        pltpu.make_async_copy(material, mat, load_sem.at[1]),
        pltpu.make_async_copy(inertial, ext.at[pl.ds(INERT, 3), own_x, own_y], load_sem.at[2]),
        pltpu.make_async_copy(start, first, load_sem.at[3]),
    ]
    for copy in loads:
        copy.start()

    def exists(offset):
        found = None
        for i, o in enumerate(offset):
            if o:
                found = has[i][o] if found is None else found & has[i][o]
        return found

    def peer(offset):
        return {AXES[i]: here[i] + o for i, o in enumerate(offset) if o}

    def back(offset):
        return tuple(-o for o in offset)

    blank = jnp.zeros((size_y, size_z), jnp.float32)

    def clear(xs, spots):
        for x in xs:
            for a in range(NARR):
                for spot in spots:
                    ext[a, x, spot * size_y : (spot + 1) * size_y] = blank

    for z in range(3):
        for group in range(2):
            for g in range(4):
                for spot in range(2):
                    if (z, spot) != (1, 0) or g in (0, 3):
                        rz[z, group, g, spot * size_y : (spot + 1) * size_y] = blank
    loop(0, HALO, lambda xs: clear(xs, (0, 1)), 2)
    loop(HALO, top, lambda xs: clear(xs, (1,)), 4)
    loop(top, planes, lambda xs: clear(xs, (0, 1)), 2)

    barrier = pltpu.get_barrier_semaphore()
    for offset in AROUND:
        @pl.when(exists(offset))
        def _(offset=offset):
            pl.semaphore_signal(
                barrier, inc=1, device_id=peer(offset), device_id_type=pl.DeviceIdType.MESH
            )

    sub = lax.broadcasted_iota(jnp.int32, (size_y, size_z), 0)
    lane = lax.broadcasted_iota(jnp.int32, (size_y, size_z), 1)
    inside = ((sub < size_y - 1) | has[1][1]) & ((lane < size_z - 1) | has[2][1])
    quarter = [stiff[i] * 0.25 for i in range(MATS)]
    block = size_z // 4

    for copy in loads:
        copy.wait()

    for h in range(2):
        packed = [blank, blank]
        for i in range(HALO):
            x = HALO * h + i
            m = mat[x]
            w = jnp.zeros((size_y, size_z), jnp.float32)
            for index in range(MATS):
                w = jnp.where(m == index, quarter[index], w)
            keep = inside if x < size_x - 1 else inside & has[0][1]
            pin = pins[x] > 0
            inert = [ext[INERT + c, x + HALO, 0:size_y] for c in range(3)]
            arrays = [jnp.where(pin, inert[c], first[c, x]) for c in range(3)]
            arrays += [jnp.where(keep, w, 0.0)] + inert + [jnp.where(pin, 1.0, 0.0)]
            for a in (0, 1, 2, WEIGHT, PIN):
                ext[a, x + HALO, 0:size_y] = arrays[a]
            for a in range(NARR):
                spot = block * (a % SPAN) + SLOT * i
                moved = pltpu.roll(arrays[a], (spot + HALO) % size_z, 1)
                mine = (lane >= spot) & (lane < spot + SLOT)
                packed[a // SPAN] = jnp.where(mine, moved, packed[a // SPAN])
        for group in range(2):
            pk[group, h] = packed[group]
            rz[1, group, 1 + h, 0:size_y] = packed[group]

    def remote(src, dst, k, offset):
        return pltpu.make_async_remote_copy(
            src_ref=src, dst_ref=dst, send_sem=send_sem.at[k], recv_sem=recv_sem.at[k],
            device_id=peer(offset), device_id_type=pl.DeviceIdType.MESH,
        )

    def row_spans(dy, depth):
        if dy == 0:
            return own_y, own_y
        if dy > 0:
            return pl.ds(size_y - depth, depth), pl.ds(rows - depth, depth)
        return pl.ds(0, depth), pl.ds(size_y, depth)

    def plane_spans(dx, depth):
        if dx == 0:
            return own_x, own_x
        if dx > 0:
            return pl.ds(top - depth, depth), pl.ds(HALO - depth, depth)
        return pl.ds(HALO, depth), pl.ds(top, depth)

    def piece(k):
        dx, dy, dz = AROUND[k]
        parts = {0: (pl.ds(0, 2), pl.ds(1, 2)), 1: (pl.ds(1, 1), pl.ds(0, 1)), -1: (pl.ds(0, 1), pl.ds(3, 1))}
        h, g = parts[dx]
        r, to = row_spans(dy, HALO)
        return remote(pk.at[:, h, r], rz.at[1 - dz, :, g, to], k, AROUND[k])

    depths = (HALO, HALO - 1)
    sides = (-1, 1)

    def face(axis, side, group):
        offset = tuple(side if i == axis else 0 for i in range(3))
        x, x_to = plane_spans(offset[0], depths[group])
        y, y_to = row_spans(offset[1], depths[group])
        span = pl.ds(SPAN * group, SPAN)
        k = FACES + 4 * axis + 2 * group + (side > 0)
        return remote(ext.at[span, x, y], ext.at[span, x_to, y_to], k, offset)

    def corner(dx, dy, group):
        x, x_to = plane_spans(dx, depths[group])
        y, y_to = row_spans(dy, depths[group])
        span = pl.ds(SPAN * group, SPAN)
        k = CORNERS + 4 * group + 2 * (dx > 0) + (dy > 0)
        if group == 0:
            return remote(ext.at[span, x, y_to], ext.at[span, x_to, y_to], k, (dx, 0, 0))
        return remote(ext.at[span, x, y], ext.at[span, x_to, y_to], k, (dx, dy, 0))

    def when(condition, action):
        pl.when(condition)(action)

    def send_face(axis, group):
        for side in sides:
            when(has[axis][side], lambda side=side: face(axis, side, group).start())

    def get_face(axis, group):
        for side in sides:
            when(has[axis][-side], lambda side=side: face(axis, side, group).wait_recv())

    def sent_face(axis, group):
        for side in sides:
            when(has[axis][side], lambda side=side: face(axis, side, group).wait_send())

    n = 1
    for i in range(3):
        n = n * (1 + has[i][-1].astype(jnp.int32) + has[i][1].astype(jnp.int32))
    pl.semaphore_wait(barrier, n - 1)

    send_face(1, 0)
    send_face(0, 0)
    for k, offset in enumerate(AROUND):
        when(exists(offset), lambda k=k: piece(k).start())
    send_face(1, 1)
    send_face(0, 1)
    for dx, dy in DIAGONAL:
        when(exists((dx, dy)), lambda dx=dx, dy=dy: corner(dx, dy, 1).start())

    get_face(1, 0)
    for dx, dy in DIAGONAL:
        when(has[0][dx] & has[1][-dy], lambda dx=dx, dy=dy: corner(dx, dy, 0).start())

    wide = lax.broadcasted_iota(jnp.int32, (rows, size_z), 1)
    edge = (wide == 0) | (wide == size_z - 1)
    up = lambda v: pltpu.roll(v, rows - 1, 0)
    down = lambda v: pltpu.roll(v, 1, 0)
    zup = lambda v: pltpu.roll(v, size_z - 1, 1)
    zdown = lambda v: pltpu.roll(v, 1, 1)
    xup = lambda v: pltpu.roll(v, size_z - SLOT, 1)
    xdown = lambda v: pltpu.roll(v, SLOT, 1)

    def make_terms(u):
        u = u * 0.25
        return node_terms(u, zup(u), up)

    def setup(xs):
        made = [(x, c, make_terms(ext[c, x])) for x in xs for c in range(3)]
        for x, c, three in made:
            for k in range(3):
                terms[x, 3 * c + k] = three[k]

    def voxels(xs):
        made = []
        for x in xs:
            low = [[terms[x, 3 * c + k] for k in range(3)] for c in range(3)]
            high = [[terms[x + 1, 3 * c + k] for k in range(3)] for c in range(3)]
            made.append((x, stress(stretch(low, high), ext[WEIGHT, x])))
        for x, p in made:
            for k in range(9):
                press[x, k] = p[k]

    def all_voxels(lo, hi):
        if (hi - lo) % 2:
            voxels([hi - 3, hi - 2, hi - 1])
            hi = hi - 3
        loop(lo, hi, voxels, 2)

    loop(HALO, top, setup, 4)
    all_voxels(HALO, top - 1)

    for k, offset in enumerate(AROUND):
        when(exists(back(offset)), lambda k=k: piece(k).wait_recv())

    late = lax.rem(wide, SLOT) >= HALO
    for group in range(2):
        for s in range(2):
            parts = [
                jnp.where(late, rz[s + 1, group, g], rz[s, group, g]) for g in range(4)
            ]
            for j in range(SPAN):
                value = None
                for g in range(4):
                    moved = parts[g]
                    if g != j:
                        moved = pltpu.roll(moved, (block * (g - j)) % size_z, 1)
                    value = moved if g == 0 else jnp.where(wide >= block * g, moved, value)
                strip[s, SPAN * group + j] = value

    def speed(total, pin):
        return jnp.where(pin > 0.0, 0.0, relax / (1.0 + 0.75 * total))

    for s in range(2):
        w = strip[s, WEIGHT]
        w = w + xdown(w)
        w = w + down(w)
        srate[s] = speed(w + zdown(w), strip[s, PIN])

    joint = lax.rem(wide, SLOT) == HALO

    def bring(low, high):
        return pltpu.roll(jnp.where(joint, low, high), size_z - HALO, 1)

    omegas = [None, 2.0 / (2.0 - radius * radius)]
    while len(omegas) < ITERS:
        omegas.append(4.0 / (4.0 - radius * radius * omegas[-1]))

    def strips(step):
        made = []
        for s in range(2):
            low, high = [], []
            for c in range(3):
                t = make_terms(strip[s, c])
                low.append(t)
                high.append([xup(v) for v in t])
            made.append(stress(stretch(low, high), strip[s, WEIGHT]))
        for c in range(3):
            sums, fresh = [], []
            for s in range(2):
                mine = made[s][3 * c : 3 * c + 3]
                minus, plus = node_sums([xdown(v) for v in mine], mine, down)
                sums.append((minus, plus))
                if step < ITERS - 1:
                    u = strip[s, c]
                    fresh.append(advance(
                        u, lambda: sprev[s, c], strip[s, INERT + c], srate[s],
                        minus + zdown(plus), omegas[step],
                    ))
                    sprev[s, c] = u
                    strip[s, c] = fresh[s]
            if step < ITERS - 1:
                zin[step, c] = bring(*fresh)
            else:
                zin[step, c] = bring(zdown(sums[0][1]), sums[1][0])

    for step in range(ITERS):
        strips(step)

    get_face(0, 0)
    for dx, dy in DIAGONAL:
        when(has[0][-dx] & has[1][-dy], lambda dx=dx, dy=dy: corner(dx, dy, 0).wait_recv())
    loop(0, HALO, setup, 4)
    loop(top, planes, setup, 4)
    all_voxels(0, HALO)
    all_voxels(top - 1, planes - 1)

    get_face(1, 1)
    get_face(0, 1)
    for dx, dy in DIAGONAL:
        when(has[0][-dx] & has[1][-dy], lambda dx=dx, dy=dy: corner(dx, dy, 1).wait_recv())

    for axis in range(2):
        sent_face(axis, 0)
    for dx, dy in DIAGONAL:
        when(has[0][dx] & has[1][-dy], lambda dx=dx, dy=dy: corner(dx, dy, 0).wait_send())

    def place(value, x):
        return pltpu.roll(value, size_z - SLOT * x, 1)

    def weigh(xs):
        made = []
        for x in xs:
            w = ext[WEIGHT, x - 1] + ext[WEIGHT, x]
            w = w + down(w)
            value = speed(w + zdown(w), ext[PIN, x])
            low = pltpu.roll(srate[0], size_z - HALO - SLOT * x + size_z, 1)
            made.append((x, jnp.where(wide == 0, low, value)))
        for x, value in made:
            rate[x] = value

    loop(1, planes - 1, weigh, (planes - 2) // 2)

    def nodes(step, xs):
        made = []
        last = step == ITERS - 1
        for x in xs:
            r = rate[x]
            for c in range(3):
                minus, plus = node_sums(
                    [press[x - 1, 3 * c + k] for k in range(3)],
                    [press[x, 3 * c + k] for k in range(3)],
                    down,
                )
                plus = zdown(plus)
                beside = place(zin[step, c], x)
                if last:
                    minus = jnp.where(wide == size_z - 1, beside, minus)
                    plus = jnp.where(wide == 0, beside, plus)
                u = ext[c, x]
                fresh = advance(
                    u, lambda: prev[c, x], ext[INERT + c, x], r, minus + plus, omegas[step]
                )
                if not last:
                    fresh = jnp.where(edge, beside, fresh)
                made.append((x, c, u, fresh))
        if last:
            for x, c, _, fresh in made:
                done[c, x - HALO] = fresh[0:size_y]
            return
        later = [(x, c, make_terms(fresh)) for x, c, _, fresh in made]
        for x, c, u, fresh in made:
            prev[c, x] = u
            ext[c, x] = fresh
        for x, c, three in later:
            for k in range(3):
                terms[x, 3 * c + k] = three[k]

    for step in range(ITERS):
        if step:
            all_voxels(step, planes - 1 - step)
        if step < ITERS - 1:
            loop(step + 1, planes - 1 - step, functools.partial(nodes, step))

    stores = []
    for h in range(2):
        loop(HALO * (h + 1), HALO * (h + 2), functools.partial(nodes, ITERS - 1), 4)
        span = pl.ds(HALO * h, HALO)
        stores.append(pltpu.make_async_copy(done.at[:, span], out.at[:, span], load_sem.at[h]))
        stores[h].start()

    for axis in range(2):
        sent_face(axis, 1)
    for k, offset in enumerate(AROUND):
        when(exists(offset), lambda k=k: piece(k).wait_send())
    for dx, dy in DIAGONAL:
        when(exists((dx, dy)), lambda dx=dx, dy=dy: corner(dx, dy, 1).wait_send())
    for copy in stores:
        copy.wait()


def per_device(counts, start_disp, inertial, material, pinned, stiffness):
    size_x, size_y, size_z = material.shape
    planes, rows = size_x + 2 * HALO, 2 * size_y
    assert planes * SLOT == size_z and size_y == 2 * HALO and size_x == 2 * HALO
    hbm = pl.BlockSpec(memory_space=pl.ANY)
    f32 = lambda *shape: pltpu.VMEM(shape, jnp.float32)
    i32 = lambda *shape: pltpu.VMEM(shape, jnp.int32)
    return pl.pallas_call(
        functools.partial(kernel, counts),
        out_shape=jax.ShapeDtypeStruct(start_disp.shape, jnp.float32),
        in_specs=[hbm, hbm, hbm, hbm, pl.BlockSpec(memory_space=pltpu.SMEM)],
        out_specs=hbm,
        scratch_shapes=[
            f32(3, size_x, size_y, size_z),
            i32(size_x, size_y, size_z),
            i32(size_x, size_y, size_z),
            f32(NARR, planes, rows, size_z),
            f32(2, 2, size_y, size_z),
            f32(3, 2, 4, rows, size_z),
            f32(2, NARR, rows, size_z),
            f32(2, 3, rows, size_z),
            f32(2, rows, size_z),
            f32(ITERS, 3, rows, size_z),
            f32(3, planes, rows, size_z),
            f32(planes, rows, size_z),
            f32(planes, 9, rows, size_z),
            f32(planes, 9, rows, size_z),
            f32(3, size_x, size_y, size_z),
            pltpu.SemaphoreType.DMA((COPIES,)),
            pltpu.SemaphoreType.DMA((COPIES,)),
            pltpu.SemaphoreType.DMA((4,)),
        ],
        compiler_params=pltpu.CompilerParams(collective_id=0, has_side_effects=True),
    )(start_disp, inertial, material, pinned, stiffness)


def solution(mesh):
    placed = (
        P(None, "gx", "gy", "gz"),
        P(None, "gx", "gy", "gz"),
        P("gx", "gy", "gz"),
        P("gx", "gy", "gz"),
        P(),
    )
    counts = tuple(mesh.shape[a] for a in AXES)
    return jax.shard_map(
        functools.partial(per_device, counts), mesh=mesh, in_specs=placed,
        out_specs=P(None, "gx", "gy", "gz"), check_vma=False,
    )
```

```python
import functools
import itertools

import jax
import jax.numpy as jnp
from jax import lax
from jax.experimental import pallas as pl
from jax.experimental.pallas import tpu as pltpu
from jax.sharding import PartitionSpec as P

ITERS = 4
POLAR_STEPS = 6
MATS = 8

relax = 0.6
radius = 0.9
HALO = ITERS
SLOT = 2 * HALO
NARR = 8
SPAN = NARR // 2
WEIGHT, INERT, PIN = 3, 4, 7
AXES = ("gx", "gy", "gz")
AROUND = tuple(o for o in itertools.product((-1, 0, 1), repeat=3) if any(o))
DIAGONAL = tuple(itertools.product((-1, 1), repeat=2))
FACES = len(AROUND)
CORNERS = FACES + 8
COPIES = CORNERS + 8


def loop(lo, hi, body, unroll=2):
    assert (hi - lo) % unroll == 0

    def group(k, _):
        body([lo + k * unroll + i for i in range(unroll)])
        return 0

    lax.fori_loop(0, (hi - lo) // unroll, group, 0)


def node_terms(u, uz, roll_y):
    zs, zd = uz + u, uz - u
    ys, yd = roll_y(zs), roll_y(zd)
    return zs + ys, ys - zs, zd + yd


def stretch(low, high):
    deform = []
    for c in range(3):
        dx = high[c][0] - low[c][0]
        dy = high[c][1] + low[c][1]
        dz = high[c][2] + low[c][2]
        row = [dx, dy, dz]
        row[c] = row[c] + 1.0
        deform.append(row)
    return deform


COSINE = (
    1.00000005, 1.15469445, -0.222086479, 0.105738212,
    -0.0606261262, 0.0323189784, -0.0123398994, 0.00230085802,
)


def stress(deform, w):
    f = deform
    s = {}
    for i in range(3):
        for j in range(i, 3):
            s[i, j] = f[0][i] * f[0][j] + f[1][i] * f[1][j] + f[2][i] * f[2][j]
    mean = (s[0, 0] + s[1, 1] + s[2, 2]) * (1.0 / 3.0)
    inv = jnp.minimum(lax.rsqrt(mean), 1.0)
    k11, k22, k33 = (s[i, i] - mean for i in range(3))
    k12, k13, k23 = s[0, 1], s[0, 2], s[1, 2]
    a11, a12, a13, a23 = k11 * k11, k12 * k12, k13 * k13, k23 * k23
    b23, c23 = k22 * k33, k12 * k13
    spread = a11 - b23 + a12 + (a13 + a23)
    spread = jnp.maximum(spread * (1.0 / 3.0), 1e-30)
    rp = lax.rsqrt(spread)
    rp2 = rp * rp
    det = k11 * (b23 - a23) - k22 * a13 + ((c23 + c23) * k23 - k33 * a12)
    half = 0.5 + 0.25 * (det * rp * rp2)
    half = jnp.minimum(jnp.maximum(half, 1e-12), 1.0)
    root = half * lax.rsqrt(half)
    e = COSINE[-1]
    for a in COSINE[-2::-1]:
        e = e * root + a
    t2 = jnp.maximum(3.0 - 0.75 * (e * e), 1e-12)
    y = lax.rsqrt(t2)
    t = t2 * y
    e2 = 0.5 * e
    e3 = e + e2
    x2, x3 = t - e2, t + e2
    r12 = 1.0 / jnp.maximum(e3 - t, 1e-6)
    r13 = 1.0 / (e3 + t)
    r23 = 0.5 * y
    scale = 0.5 * (inv * inv)
    p = spread * rp * scale
    mean = mean * scale
    inv = inv * w
    qs = []
    for h in (mean + p * e, mean + p * x2, mean - p * x3):
        m = 1.5 - h
        q = inv * m
        for _ in range(POLAR_STEPS - 1):
            h = h * (m * m)
            m = 1.5 - h
            q = q * m
        qs.append(q)
    q12 = (qs[0] - qs[1]) * r12
    q23 = (qs[1] - qs[2]) * r23
    c2 = (q12 - q23) * r13
    c0 = (w - qs[0]) + (q12 * e - c2 * (e * x2))
    c1 = (c2 * x3 - q12) * rp
    c2 = c2 * rp2
    g = {
        (0, 0): (c0 + c1 * k11) - c2 * (a11 + (a12 + a13)),
        (1, 1): (c0 + c1 * k22) - c2 * (k22 * k22 + (a12 + a23)),
        (2, 2): (c0 + c1 * k33) - c2 * (k33 * k33 + (a13 + a23)),
        (0, 1): c1 * k12 - c2 * (k13 * k23 - k12 * k33),
        (0, 2): c1 * k13 - c2 * (k12 * k23 - k13 * k22),
        (1, 2): c1 * k23 - c2 * (c23 - k23 * k11),
    }
    pick = lambda i, j: g[min(i, j), max(i, j)]
    return [
        f[c][0] * pick(0, d) + f[c][1] * pick(1, d) + f[c][2] * pick(2, d)
        for c in range(3) for d in range(3)
    ]


def node_sums(before, here, roll_y):
    a = before[0] - here[0]
    b = before[1] + here[1]
    e = before[2] + here[2]
    g = (a - b) + roll_y(a + b)
    e = e + roll_y(e)
    return g - e, g + e


def advance(u, prev, inert, rate, f, omega):
    target = u - rate * ((u - inert) + f)
    return target if omega is None else omega * (target - prev()) + prev()


def kernel(
    counts, start, inertial, material, pinned, stiff, out,
    first, mat, pins, ext, pk, rz, strip, sprev, srate, zin, prev, rate, terms, press,
    send_sem, recv_sem, load_sem,
):
    size_x, size_y, size_z = material.shape
    top = HALO + size_x
    planes = top + HALO
    rows = 2 * size_y
    own_y, own_x = pl.ds(0, size_y), pl.ds(HALO, size_x)
    here = [lax.axis_index(a) for a in AXES]
    has = [{-1: here[i] > 0, 1: here[i] < counts[i] - 1} for i in range(3)]

    loads = [
        pltpu.make_async_copy(pinned, pins, load_sem.at[0]),
        pltpu.make_async_copy(material, mat, load_sem.at[1]),
        pltpu.make_async_copy(inertial, ext.at[pl.ds(INERT, 3), own_x, own_y], load_sem.at[2]),
        pltpu.make_async_copy(start, first, load_sem.at[3]),
    ]
    for copy in loads:
        copy.start()

    def exists(offset):
        found = None
        for i, o in enumerate(offset):
            if o:
                found = has[i][o] if found is None else found & has[i][o]
        return found

    def peer(offset):
        return {AXES[i]: here[i] + o for i, o in enumerate(offset) if o}

    def back(offset):
        return tuple(-o for o in offset)

    blank = jnp.zeros((size_y, size_z), jnp.float32)

    def clear(xs, spots):
        for x in xs:
            for a in range(NARR):
                for spot in spots:
                    ext[a, x, spot * size_y : (spot + 1) * size_y] = blank

    for z in range(3):
        for group in range(2):
            for g in range(4):
                for spot in range(2):
                    if (z, spot) != (1, 0) or g in (0, 3):
                        rz[z, group, g, spot * size_y : (spot + 1) * size_y] = blank
    loop(0, HALO, lambda xs: clear(xs, (0, 1)), 2)
    loop(HALO, top, lambda xs: clear(xs, (1,)), 4)
    loop(top, planes, lambda xs: clear(xs, (0, 1)), 2)

    barrier = pltpu.get_barrier_semaphore()
    for offset in AROUND:
        @pl.when(exists(offset))
        def _(offset=offset):
            pl.semaphore_signal(
                barrier, inc=1, device_id=peer(offset), device_id_type=pl.DeviceIdType.MESH
            )

    sub = lax.broadcasted_iota(jnp.int32, (size_y, size_z), 0)
    lane = lax.broadcasted_iota(jnp.int32, (size_y, size_z), 1)
    inside = ((sub < size_y - 1) | has[1][1]) & ((lane < size_z - 1) | has[2][1])
    quarter = [stiff[i] * 0.25 for i in range(MATS)]
    block = size_z // 4

    for copy in loads:
        copy.wait()

    for h in range(2):
        packed = [blank, blank]
        for i in range(HALO):
            x = HALO * h + i
            m = mat[x]
            w = jnp.zeros((size_y, size_z), jnp.float32)
            for index in range(MATS):
                w = jnp.where(m == index, quarter[index], w)
            keep = inside if x < size_x - 1 else inside & has[0][1]
            pin = pins[x] > 0
            inert = [ext[INERT + c, x + HALO, 0:size_y] for c in range(3)]
            arrays = [jnp.where(pin, inert[c], first[c, x]) for c in range(3)]
            arrays += [jnp.where(keep, w, 0.0)] + inert + [jnp.where(pin, 1.0, 0.0)]
            for a in (0, 1, 2, WEIGHT, PIN):
                ext[a, x + HALO, 0:size_y] = arrays[a]
            for a in range(NARR):
                spot = block * (a % SPAN) + SLOT * i
                moved = pltpu.roll(arrays[a], (spot + HALO) % size_z, 1)
                mine = (lane >= spot) & (lane < spot + SLOT)
                packed[a // SPAN] = jnp.where(mine, moved, packed[a // SPAN])
        for group in range(2):
            pk[group, h] = packed[group]
            rz[1, group, 1 + h, 0:size_y] = packed[group]

    def remote(src, dst, k, offset):
        return pltpu.make_async_remote_copy(
            src_ref=src, dst_ref=dst, send_sem=send_sem.at[k], recv_sem=recv_sem.at[k],
            device_id=peer(offset), device_id_type=pl.DeviceIdType.MESH,
        )

    def row_spans(dy, depth):
        if dy == 0:
            return own_y, own_y
        if dy > 0:
            return pl.ds(size_y - depth, depth), pl.ds(rows - depth, depth)
        return pl.ds(0, depth), pl.ds(size_y, depth)

    def plane_spans(dx, depth):
        if dx == 0:
            return own_x, own_x
        if dx > 0:
            return pl.ds(top - depth, depth), pl.ds(HALO - depth, depth)
        return pl.ds(HALO, depth), pl.ds(top, depth)

    def piece(k):
        dx, dy, dz = AROUND[k]
        parts = {0: (pl.ds(0, 2), pl.ds(1, 2)), 1: (pl.ds(1, 1), pl.ds(0, 1)), -1: (pl.ds(0, 1), pl.ds(3, 1))}
        h, g = parts[dx]
        r, to = row_spans(dy, HALO)
        return remote(pk.at[:, h, r], rz.at[1 - dz, :, g, to], k, AROUND[k])

    depths = (HALO, HALO - 1)
    sides = (-1, 1)

    def face(axis, side, group):
        offset = tuple(side if i == axis else 0 for i in range(3))
        x, x_to = plane_spans(offset[0], depths[group])
        y, y_to = row_spans(offset[1], depths[group])
        span = pl.ds(SPAN * group, SPAN)
        k = FACES + 4 * axis + 2 * group + (side > 0)
        return remote(ext.at[span, x, y], ext.at[span, x_to, y_to], k, offset)

    def corner(dx, dy, group):
        x, x_to = plane_spans(dx, depths[group])
        y, y_to = row_spans(dy, depths[group])
        span = pl.ds(SPAN * group, SPAN)
        k = CORNERS + 4 * group + 2 * (dx > 0) + (dy > 0)
        if group == 0:
            return remote(ext.at[span, x, y_to], ext.at[span, x_to, y_to], k, (dx, 0, 0))
        return remote(ext.at[span, x, y], ext.at[span, x_to, y_to], k, (dx, dy, 0))

    def when(condition, action):
        pl.when(condition)(action)

    def send_face(axis, group):
        for side in sides:
            when(has[axis][side], lambda side=side: face(axis, side, group).start())

    def get_face(axis, group):
        for side in sides:
            when(has[axis][-side], lambda side=side: face(axis, side, group).wait_recv())

    def sent_face(axis, group):
        for side in sides:
            when(has[axis][side], lambda side=side: face(axis, side, group).wait_send())

    n = 1
    for i in range(3):
        n = n * (1 + has[i][-1].astype(jnp.int32) + has[i][1].astype(jnp.int32))
    pl.semaphore_wait(barrier, n - 1)

    send_face(1, 0)
    send_face(0, 0)
    for k, offset in enumerate(AROUND):
        when(exists(offset), lambda k=k: piece(k).start())
    send_face(1, 1)
    send_face(0, 1)
    for dx, dy in DIAGONAL:
        when(exists((dx, dy)), lambda dx=dx, dy=dy: corner(dx, dy, 1).start())

    get_face(1, 0)
    for dx, dy in DIAGONAL:
        when(has[0][dx] & has[1][-dy], lambda dx=dx, dy=dy: corner(dx, dy, 0).start())

    wide = lax.broadcasted_iota(jnp.int32, (rows, size_z), 1)
    edge = (wide == 0) | (wide == size_z - 1)
    up = lambda v: pltpu.roll(v, rows - 1, 0)
    down = lambda v: pltpu.roll(v, 1, 0)
    zup = lambda v: pltpu.roll(v, size_z - 1, 1)
    zdown = lambda v: pltpu.roll(v, 1, 1)
    xup = lambda v: pltpu.roll(v, size_z - SLOT, 1)
    xdown = lambda v: pltpu.roll(v, SLOT, 1)

    def make_terms(u):
        u = u * 0.25
        return node_terms(u, zup(u), up)

    def setup(xs):
        made = [(x, c, make_terms(ext[c, x])) for x in xs for c in range(3)]
        for x, c, three in made:
            for k in range(3):
                terms[x, 3 * c + k] = three[k]

    def voxels(xs):
        made = []
        for x in xs:
            low = [[terms[x, 3 * c + k] for k in range(3)] for c in range(3)]
            high = [[terms[x + 1, 3 * c + k] for k in range(3)] for c in range(3)]
            made.append((x, stress(stretch(low, high), ext[WEIGHT, x])))
        for x, p in made:
            for k in range(9):
                press[x, k] = p[k]

    def all_voxels(lo, hi):
        if (hi - lo) % 2:
            voxels([hi - 3, hi - 2, hi - 1])
            hi = hi - 3
        loop(lo, hi, voxels, 2)

    loop(HALO, top, setup, SLOT)
    all_voxels(HALO, top - 1)

    for k, offset in enumerate(AROUND):
        when(exists(back(offset)), lambda k=k: piece(k).wait_recv())

    late = lax.rem(wide, SLOT) >= HALO
    for group in range(2):
        for s in range(2):
            parts = [
                jnp.where(late, rz[s + 1, group, g], rz[s, group, g]) for g in range(4)
            ]
            for j in range(SPAN):
                value = None
                for g in range(4):
                    moved = parts[g]
                    if g != j:
                        moved = pltpu.roll(moved, (block * (g - j)) % size_z, 1)
                    value = moved if g == 0 else jnp.where(wide >= block * g, moved, value)
                strip[s, SPAN * group + j] = value

    def speed(total, pin):
        return jnp.where(pin > 0.0, 0.0, relax / (1.0 + 0.75 * total))

    for s in range(2):
        w = strip[s, WEIGHT]
        w = w + xdown(w)
        w = w + down(w)
        srate[s] = speed(w + zdown(w), strip[s, PIN])

    joint = lax.rem(wide, SLOT) == HALO

    def bring(low, high):
        return pltpu.roll(jnp.where(joint, low, high), size_z - HALO, 1)

    omegas = [None, 2.0 / (2.0 - radius * radius)]
    while len(omegas) < ITERS:
        omegas.append(4.0 / (4.0 - radius * radius * omegas[-1]))

    def strips(step):
        made = []
        for s in range(2):
            low, high = [], []
            for c in range(3):
                u = strip[s, c] * 0.25
                low.append(node_terms(u, zup(u), up))
                high.append(node_terms(xup(u), pltpu.roll(u, size_z - SLOT - 1, 1), up))
            made.append(stress(stretch(low, high), strip[s, WEIGHT]))
        for c in range(3):
            fresh = []
            for s in range(2):
                a, b, e = made[s][3 * c : 3 * c + 3]
                both, less = a + b, a - b
                e = e + down(e)
                here, before = down(-less) - both, less + down(both)
                last = step == ITERS - 1
                if not last:
                    u = strip[s, c]
                    f = (here - e) + xdown(before - e)
                    f = f + (zdown(here + e) + pltpu.roll(before + e, SLOT + 1, 1))
                    fresh.append(advance(
                        u, lambda: sprev[s, c], strip[s, INERT + c], srate[s], f, omegas[step]
                    ))
                    sprev[s, c] = u
                    strip[s, c] = fresh[s]
                elif s == 0:
                    fresh.append(zdown(here + e) + pltpu.roll(before + e, SLOT + 1, 1))
                else:
                    fresh.append((here - e) + xdown(before - e))
            zin[step, c] = bring(*fresh)

    for step in range(ITERS):
        strips(step)

    get_face(0, 0)
    for dx, dy in DIAGONAL:
        when(has[0][-dx] & has[1][-dy], lambda dx=dx, dy=dy: corner(dx, dy, 0).wait_recv())
    loop(0, HALO, setup, 4)
    loop(top, planes, setup, 4)
    all_voxels(0, HALO)
    all_voxels(top - 1, planes - 1)

    get_face(1, 1)
    get_face(0, 1)
    for dx, dy in DIAGONAL:
        when(has[0][-dx] & has[1][-dy], lambda dx=dx, dy=dy: corner(dx, dy, 1).wait_recv())

    for axis in range(2):
        sent_face(axis, 0)
    for dx, dy in DIAGONAL:
        when(has[0][dx] & has[1][-dy], lambda dx=dx, dy=dy: corner(dx, dy, 0).wait_send())

    def place(value, x):
        return pltpu.roll(value, size_z - SLOT * x, 1)

    def weigh(xs):
        made = []
        for x in xs:
            w = ext[WEIGHT, x - 1] + ext[WEIGHT, x]
            w = w + down(w)
            value = speed(w + zdown(w), ext[PIN, x])
            low = pltpu.roll(srate[0], size_z - HALO - SLOT * x + size_z, 1)
            made.append((x, jnp.where(wide == 0, low, value)))
        for x, value in made:
            rate[x] = value

    loop(1, planes - 1, weigh, (planes - 2) // 2)

    def nodes(step, xs):
        made = []
        last = step == ITERS - 1
        for x in xs:
            r = rate[x]
            for c in range(3):
                minus, plus = node_sums(
                    [press[x - 1, 3 * c + k] for k in range(3)],
                    [press[x, 3 * c + k] for k in range(3)],
                    down,
                )
                plus = zdown(plus)
                beside = place(zin[step, c], x)
                if last:
                    minus = jnp.where(wide == size_z - 1, beside, minus)
                    plus = jnp.where(wide == 0, beside, plus)
                u = ext[c, x]
                fresh = advance(
                    u, lambda: prev[c, x], ext[INERT + c, x], r, minus + plus, omegas[step]
                )
                if not last:
                    fresh = jnp.where(edge, beside, fresh)
                made.append((x, c, u, fresh))
        if last:
            for x, c, _, fresh in made:
                out[c, x - HALO] = fresh[0:size_y]
            return
        later = [(x, c, make_terms(fresh)) for x, c, _, fresh in made]
        for x, c, u, fresh in made:
            prev[c, x] = u
            ext[c, x] = fresh
        for x, c, three in later:
            for k in range(3):
                terms[x, 3 * c + k] = three[k]

    for step in range(ITERS):
        if step:
            all_voxels(step, planes - 1 - step)
        if step < ITERS - 1:
            loop(step + 1, planes - 1 - step, functools.partial(nodes, step), SLOT - 1 - step)

    loop(HALO, top, functools.partial(nodes, ITERS - 1), HALO)

    for axis in range(2):
        sent_face(axis, 1)
    for k, offset in enumerate(AROUND):
        when(exists(offset), lambda k=k: piece(k).wait_send())
    for dx, dy in DIAGONAL:
        when(exists((dx, dy)), lambda dx=dx, dy=dy: corner(dx, dy, 1).wait_send())


def per_device(counts, start_disp, inertial, material, pinned, stiffness):
    size_x, size_y, size_z = material.shape
    planes, rows = size_x + 2 * HALO, 2 * size_y
    assert planes * SLOT == size_z and size_y == 2 * HALO and size_x == 2 * HALO
    hbm = pl.BlockSpec(memory_space=pl.ANY)
    f32 = lambda *shape: pltpu.VMEM(shape, jnp.float32)
    i32 = lambda *shape: pltpu.VMEM(shape, jnp.int32)
    return pl.pallas_call(
        functools.partial(kernel, counts),
        out_shape=pltpu.VMEM(start_disp.shape, jnp.float32),
        in_specs=[hbm, hbm, hbm, hbm, pl.BlockSpec(memory_space=pltpu.SMEM)],
        out_specs=pl.BlockSpec(memory_space=pltpu.VMEM),
        scratch_shapes=[
            f32(3, size_x, size_y, size_z),
            i32(size_x, size_y, size_z),
            i32(size_x, size_y, size_z),
            f32(NARR, planes, rows, size_z),
            f32(2, 2, size_y, size_z),
            f32(3, 2, 4, rows, size_z),
            f32(2, NARR, rows, size_z),
            f32(2, 3, rows, size_z),
            f32(2, rows, size_z),
            f32(ITERS, 3, rows, size_z),
            f32(3, planes, rows, size_z),
            f32(planes, rows, size_z),
            f32(planes, 9, rows, size_z),
            f32(planes, 9, rows, size_z),
            pltpu.SemaphoreType.DMA((COPIES,)),
            pltpu.SemaphoreType.DMA((COPIES,)),
            pltpu.SemaphoreType.DMA((4,)),
        ],
        compiler_params=pltpu.CompilerParams(collective_id=0, has_side_effects=True),
    )(start_disp, inertial, material, pinned, stiffness)


def solution(mesh):
    placed = (
        P(None, "gx", "gy", "gz"),
        P(None, "gx", "gy", "gz"),
        P("gx", "gy", "gz"),
        P("gx", "gy", "gz"),
        P(),
    )
    counts = tuple(mesh.shape[a] for a in AXES)
    return jax.shard_map(
        functools.partial(per_device, counts), mesh=mesh, in_specs=placed,
        out_specs=P(None, "gx", "gy", "gz"), check_vma=False,
    )
```

```python
import functools
import itertools

import jax
import jax.numpy as jnp
from jax import lax
from jax.experimental import pallas as pl
from jax.experimental.pallas import tpu as pltpu
from jax.sharding import PartitionSpec as P

ITERS = 4
POLAR_STEPS = 6
MATS = 8

relax = 0.6
radius = 0.9
HALO = ITERS
SLOT = 2 * HALO
NARR = 8
SPAN = NARR // 2
WEIGHT, INERT, PIN = 3, 4, 7
AXES = ("gx", "gy", "gz")
AROUND = tuple(o for o in itertools.product((-1, 0, 1), repeat=3) if any(o))
DIAGONAL = tuple(itertools.product((-1, 1), repeat=2))
SENT, PIECES, HALVES, NEAR, FAR = 0, 1, 2, 4, 5


def loop(lo, hi, body, unroll=2):
    assert (hi - lo) % unroll == 0

    def group(k, _):
        body([lo + k * unroll + i for i in range(unroll)])
        return 0

    lax.fori_loop(0, (hi - lo) // unroll, group, 0)


def node_terms(u, uz, roll_y):
    zs, zd = uz + u, uz - u
    ys, yd = roll_y(zs), roll_y(zd)
    return zs + ys, ys - zs, zd + yd


def stretch(low, high):
    deform = []
    for c in range(3):
        dx = high[c][0] - low[c][0]
        dy = high[c][1] + low[c][1]
        dz = high[c][2] + low[c][2]
        row = [dx, dy, dz]
        row[c] = row[c] + 1.0
        deform.append(row)
    return deform


COSINE = (
    1.00000005, 1.15469445, -0.222086479, 0.105738212,
    -0.0606261262, 0.0323189784, -0.0123398994, 0.00230085802,
)


def stress(deform, w):
    f = deform
    s = {}
    for i in range(3):
        for j in range(i, 3):
            s[i, j] = f[0][i] * f[0][j] + f[1][i] * f[1][j] + f[2][i] * f[2][j]
    mean = (s[0, 0] + s[1, 1] + s[2, 2]) * (1.0 / 3.0)
    inv = jnp.minimum(lax.rsqrt(mean), 1.0)
    k11, k22, k33 = (s[i, i] - mean for i in range(3))
    k12, k13, k23 = s[0, 1], s[0, 2], s[1, 2]
    a11, a12, a13, a23 = k11 * k11, k12 * k12, k13 * k13, k23 * k23
    b23, c23 = k22 * k33, k12 * k13
    spread = a11 - b23 + a12 + (a13 + a23)
    spread = jnp.maximum(spread * (1.0 / 3.0), 1e-30)
    rp = lax.rsqrt(spread)
    rp2 = rp * rp
    det = k11 * (b23 - a23) - k22 * a13 + ((c23 + c23) * k23 - k33 * a12)
    half = 0.5 + 0.25 * (det * rp * rp2)
    half = jnp.minimum(jnp.maximum(half, 1e-12), 1.0)
    root = half * lax.rsqrt(half)
    e = COSINE[-1]
    for a in COSINE[-2::-1]:
        e = e * root + a
    t2 = jnp.maximum(3.0 - 0.75 * (e * e), 1e-12)
    y = lax.rsqrt(t2)
    t = t2 * y
    e2 = 0.5 * e
    e3 = e + e2
    x2, x3 = t - e2, t + e2
    r12 = 1.0 / jnp.maximum(e3 - t, 1e-6)
    r13 = 1.0 / (e3 + t)
    r23 = 0.5 * y
    scale = 0.5 * (inv * inv)
    p = spread * rp * scale
    mean = mean * scale
    inv = inv * w
    qs = []
    for h in (mean + p * e, mean + p * x2, mean - p * x3):
        m = 1.5 - h
        q = inv * m
        for _ in range(POLAR_STEPS - 1):
            h = h * (m * m)
            m = 1.5 - h
            q = q * m
        qs.append(q)
    q12 = (qs[0] - qs[1]) * r12
    q23 = (qs[1] - qs[2]) * r23
    c2 = (q12 - q23) * r13
    c0 = (w - qs[0]) + (q12 * e - c2 * (e * x2))
    c1 = (c2 * x3 - q12) * rp
    c2 = c2 * rp2
    g = {
        (0, 0): (c0 + c1 * k11) - c2 * (a11 + (a12 + a13)),
        (1, 1): (c0 + c1 * k22) - c2 * (k22 * k22 + (a12 + a23)),
        (2, 2): (c0 + c1 * k33) - c2 * (k33 * k33 + (a13 + a23)),
        (0, 1): c1 * k12 - c2 * (k13 * k23 - k12 * k33),
        (0, 2): c1 * k13 - c2 * (k12 * k23 - k13 * k22),
        (1, 2): c1 * k23 - c2 * (c23 - k23 * k11),
    }
    pick = lambda i, j: g[min(i, j), max(i, j)]
    return [
        f[c][0] * pick(0, d) + f[c][1] * pick(1, d) + f[c][2] * pick(2, d)
        for c in range(3) for d in range(3)
    ]


def node_sums(before, here, roll_y):
    a = before[0] - here[0]
    b = before[1] + here[1]
    e = before[2] + here[2]
    g = (a - b) + roll_y(a + b)
    e = e + roll_y(e)
    return g - e, g + e


def advance(u, prev, inert, rate, f, omega):
    target = u - rate * ((u - inert) + f)
    return target if omega is None else omega * (target - prev()) + prev()


def kernel(
    counts, start, inertial, material, pinned, stiffness, out,
    stiff, first, mat, pins, ext, pk, rz, strip, sprev, srate, zin, prev, rate, terms, press,
    spare, copy_sem, load_sem,
):
    size_x, size_y, size_z = material.shape
    top = HALO + size_x
    planes = top + HALO
    rows = 2 * size_y
    own_y, own_x = pl.ds(0, size_y), pl.ds(HALO, size_x)
    here = [lax.axis_index(a) for a in AXES]
    has = [{-1: here[i] > 0, 1: here[i] < counts[i] - 1} for i in range(3)]

    loads = [
        pltpu.make_async_copy(pinned, pins, load_sem.at[0]),
        pltpu.make_async_copy(material, mat, load_sem.at[0]),
        pltpu.make_async_copy(inertial, ext.at[pl.ds(INERT, 3), own_x, own_y], load_sem.at[0]),
        pltpu.make_async_copy(start, first, load_sem.at[0]),
        pltpu.make_async_copy(stiffness, stiff, load_sem.at[1]),
    ]
    for copy in loads:
        copy.start()

    def exists(offset):
        found = None
        for i, o in enumerate(offset):
            if o:
                found = has[i][o] if found is None else found & has[i][o]
        return found

    def peer(offset):
        return {AXES[i]: here[i] + o for i, o in enumerate(offset) if o}

    blank = jnp.zeros((size_y, size_z), jnp.float32)

    def clear(xs, spots):
        for x in xs:
            for a in range(NARR):
                for spot in spots:
                    ext[a, x, spot * size_y : (spot + 1) * size_y] = blank

    def slot(z, spot, g, group):
        return 2 * (4 * (2 * z + spot) + g) + group

    for z in range(3):
        for spot in range(2):
            for g in range(4):
                if (z, spot) != (1, 0) or g in (0, 3):
                    for group in range(2):
                        rz[slot(z, spot, g, group)] = blank
    loop(0, HALO, lambda xs: clear(xs, (0, 1)), 2)
    loop(HALO, top, lambda xs: clear(xs, (1,)), 4)
    loop(top, planes, lambda xs: clear(xs, (0, 1)), 2)

    barrier = pltpu.get_barrier_semaphore()
    for offset in AROUND:
        @pl.when(exists(offset))
        def _(offset=offset):
            pl.semaphore_signal(
                barrier, inc=1, device_id=peer(offset), device_id_type=pl.DeviceIdType.MESH
            )

    sub = lax.broadcasted_iota(jnp.int32, (size_y, size_z), 0)
    lane = lax.broadcasted_iota(jnp.int32, (size_y, size_z), 1)
    inside = ((sub < size_y - 1) | has[1][1]) & ((lane < size_z - 1) | has[2][1])
    block = size_z // 4

    part = spare.at[pl.ds(0, 8 * size_x)]
    pltpu.make_async_copy(part, part, load_sem.at[0]).wait()
    loads[-1].wait()
    quarter = [stiff[i] * 0.25 for i in range(MATS)]

    for h in range(2):
        packed = [blank, blank]
        for i in range(HALO):
            x = HALO * h + i
            m = mat[x]
            w = jnp.zeros((size_y, size_z), jnp.float32)
            for index in range(MATS):
                w = jnp.where(m == index, quarter[index], w)
            keep = inside if x < size_x - 1 else inside & has[0][1]
            pin = pins[x] > 0
            inert = [ext[INERT + c, x + HALO, 0:size_y] for c in range(3)]
            arrays = [jnp.where(pin, inert[c], first[c, x]) for c in range(3)]
            arrays += [jnp.where(keep, w, 0.0)] + inert + [jnp.where(pin, 1.0, 0.0)]
            for a in (0, 1, 2, WEIGHT, PIN):
                ext[a, x + HALO, 0:size_y] = arrays[a]
            for a in range(NARR):
                spot = block * (a % SPAN) + SLOT * i
                moved = pltpu.roll(arrays[a], (spot + HALO) % size_z, 1)
                mine = (lane >= spot) & (lane < spot + SLOT)
                packed[a // SPAN] = jnp.where(mine, moved, packed[a // SPAN])
        for group in range(2):
            pk[2 * h + group] = packed[group]
            rz[slot(1, 0, 1 + h, group)] = packed[group]

    def remote(src, dst, k, offset):
        return pltpu.make_async_remote_copy(
            src_ref=src, dst_ref=dst, send_sem=copy_sem.at[SENT], recv_sem=copy_sem.at[k],
            device_id=peer(offset), device_id_type=pl.DeviceIdType.MESH,
        )

    def row_spans(dy, depth):
        if dy == 0:
            return own_y, own_y
        if dy > 0:
            return pl.ds(size_y - depth, depth), pl.ds(rows - depth, depth)
        return pl.ds(0, depth), pl.ds(size_y, depth)

    def plane_spans(dx, depth):
        if dx == 0:
            return own_x, own_x
        if dx > 0:
            return pl.ds(top - depth, depth), pl.ds(HALO - depth, depth)
        return pl.ds(HALO, depth), pl.ds(top, depth)

    def piece(offset):
        dx, dy, dz = offset
        h, g, n = {0: (0, 1, 2), 1: (1, 0, 1), -1: (0, 3, 1)}[dx]
        r, _ = row_spans(dy, HALO)
        to = slot(1 - dz, abs(dy), g, 0)
        return remote(pk.at[pl.ds(2 * h, 2 * n), r], rz.at[pl.ds(to, 2 * n), r], PIECES, offset)

    depths = (HALO, HALO - 1)
    sides = (-1, 1)

    def face(axis, side, group):
        offset = tuple(side if i == axis else 0 for i in range(3))
        x, x_to = plane_spans(offset[0], depths[group])
        y, y_to = row_spans(offset[1], depths[group])
        span = pl.ds(SPAN * group, SPAN)
        return remote(ext.at[span, x, y], ext.at[span, x_to, y_to], (NEAR, FAR)[group], offset)

    def half(side, part):
        x = pl.ds(HALO * (1 + part), HALO)
        y, y_to = row_spans(side, HALO)
        span = pl.ds(0, SPAN)
        return remote(ext.at[span, x, y], ext.at[span, x, y_to], HALVES + part, (0, side, 0))

    def corner(dx, dy, group):
        x, x_to = plane_spans(dx, depths[group])
        y, y_to = row_spans(dy, HALO)
        span = pl.ds(SPAN * group, SPAN)
        if group == 0:
            return remote(ext.at[span, x, y_to], ext.at[span, x_to, y_to], NEAR, (dx, 0, 0))
        return remote(ext.at[span, x, y], ext.at[span, x_to, y_to], FAR, (dx, dy, 0))

    def when(condition, action):
        pl.when(condition)(action)

    def send_face(axis, group):
        for side in sides:
            when(has[axis][side], lambda side=side: face(axis, side, group).start())

    near = lambda nx, ny, nz: 16 * nx + 8 * nx * ny
    far = lambda nx, ny, nz: 12 * nx + 12 * ny + 6 * nx * ny
    halves = lambda nx, ny, nz: 8 * ny
    pieces = lambda nx, ny, nz: (2 + nx) * (2 + ny) * (1 + nz) - 4

    def sent(*n):
        return pieces(*n) + 2 * halves(*n) + near(*n) + far(*n)

    beside = [has[i][-1].astype(jnp.int32) + has[i][1].astype(jnp.int32) for i in range(3)]
    choices = list(itertools.product(*[sorted({min(n - 1, 1), min(n - 1, 2)}) for n in counts]))

    def drain(k, tiles):
        for sizes in sorted({tiles(*n) for n in choices}):
            if not sizes:
                continue
            found = None
            for n in choices:
                if tiles(*n) == sizes:
                    same = (beside[0] == n[0]) & (beside[1] == n[1]) & (beside[2] == n[2])
                    found = same if found is None else found | same

            @pl.when(found)
            def _(sizes=sizes):
                part = spare.at[pl.ds(0, sizes)]
                pltpu.make_async_copy(part, part, copy_sem.at[k]).wait()

    pl.semaphore_wait(barrier, (1 + beside[0]) * (1 + beside[1]) * (1 + beside[2]) - 1)

    for part in range(2):
        for side in sides:
            when(has[1][side], lambda side=side, part=part: half(side, part).start())
    send_face(0, 0)
    for offset in AROUND:
        when(exists(offset), lambda offset=offset: piece(offset).start())
    send_face(1, 1)
    send_face(0, 1)

    for part, dx in enumerate(sides):
        drain(HALVES + part, halves)
        for dy in sides:
            when(has[0][dx] & has[1][-dy], lambda dx=dx, dy=dy: corner(dx, dy, 0).start())
    for dx, dy in DIAGONAL:
        when(exists((dx, dy)), lambda dx=dx, dy=dy: corner(dx, dy, 1).start())

    wide = lax.broadcasted_iota(jnp.int32, (rows, size_z), 1)
    edge = (wide == 0) | (wide == size_z - 1)
    up = lambda v: pltpu.roll(v, rows - 1, 0)
    down = lambda v: pltpu.roll(v, 1, 0)
    zup = lambda v: pltpu.roll(v, size_z - 1, 1)
    zdown = lambda v: pltpu.roll(v, 1, 1)
    xup = lambda v: pltpu.roll(v, size_z - SLOT, 1)
    xdown = lambda v: pltpu.roll(v, SLOT, 1)

    def make_terms(u):
        u = u * 0.25
        return node_terms(u, zup(u), up)

    def setup(xs):
        made = [(x, c, make_terms(ext[c, x])) for x in xs for c in range(3)]
        for x, c, three in made:
            for k in range(3):
                terms[x, 3 * c + k] = three[k]

    def voxels(xs):
        made = []
        for x in xs:
            low = [[terms[x, 3 * c + k] for k in range(3)] for c in range(3)]
            high = [[terms[x + 1, 3 * c + k] for k in range(3)] for c in range(3)]
            made.append((x, stress(stretch(low, high), ext[WEIGHT, x])))
        for x, p in made:
            for k in range(9):
                press[x, k] = p[k]

    def all_voxels(lo, hi):
        if (hi - lo) % 2:
            voxels([hi - 3, hi - 2, hi - 1])
            hi = hi - 3
        loop(lo, hi, voxels, 2)

    def weigh(xs):
        made = []
        for x in xs:
            w = ext[WEIGHT, x - 1] + ext[WEIGHT, x]
            w = w + down(w)
            made.append((x, relax / (1.0 + 0.75 * (w + zdown(w)))))
        for x, value in made:
            rate[x] = value

    own = list(range(HALO, top))
    weigh(own[1:])
    loop(HALO, top, setup, SLOT)
    all_voxels(HALO, top - 1)

    drain(PIECES, pieces)

    late = lax.rem(lane, SLOT) >= HALO
    for group in range(2):
        for s in range(2):
            for spot in range(2):
                parts = [
                    jnp.where(
                        late, rz[slot(s + 1, spot, g, group)], rz[slot(s, spot, g, group)]
                    )
                    for g in range(4)
                ]
                for j in range(SPAN):
                    value = None
                    for g in range(4):
                        moved = parts[g]
                        if g != j:
                            moved = pltpu.roll(moved, (block * (g - j)) % size_z, 1)
                        value = moved if g == 0 else jnp.where(lane >= block * g, moved, value)
                    strip[s, SPAN * group + j, size_y * spot : size_y * (spot + 1)] = value

    def speed(total, pin):
        return jnp.where(pin > 0.0, 0.0, relax / (1.0 + 0.75 * total))

    for s in range(2):
        w = strip[s, WEIGHT]
        w = w + xdown(w)
        w = w + down(w)
        srate[s] = speed(w + zdown(w), strip[s, PIN])

    joint = lax.rem(wide, SLOT) == HALO

    def bring(low, high):
        return pltpu.roll(jnp.where(joint, low, high), size_z - HALO, 1)

    omegas = [None, 2.0 / (2.0 - radius * radius)]
    while len(omegas) < ITERS:
        omegas.append(4.0 / (4.0 - radius * radius * omegas[-1]))

    def strips(step):
        made = []
        for s in range(2):
            low, high = [], []
            for c in range(3):
                u = strip[s, c] * 0.25
                low.append(node_terms(u, zup(u), up))
                high.append(node_terms(xup(u), pltpu.roll(u, size_z - SLOT - 1, 1), up))
            made.append(stress(stretch(low, high), strip[s, WEIGHT]))
        for c in range(3):
            fresh = []
            for s in range(2):
                a, b, e = made[s][3 * c : 3 * c + 3]
                both, less = a + b, a - b
                e = e + down(e)
                here, before = down(-less) - both, less + down(both)
                last = step == ITERS - 1
                if not last:
                    u = strip[s, c]
                    f = (here - e) + xdown(before - e)
                    f = f + (zdown(here + e) + pltpu.roll(before + e, SLOT + 1, 1))
                    fresh.append(advance(
                        u, lambda: sprev[s, c], strip[s, INERT + c], srate[s], f, omegas[step]
                    ))
                    sprev[s, c] = u
                    strip[s, c] = fresh[s]
                elif s == 0:
                    fresh.append(zdown(here + e) + pltpu.roll(before + e, SLOT + 1, 1))
                else:
                    fresh.append((here - e) + xdown(before - e))
            zin[step, c] = bring(*fresh)

    for step in range(ITERS - 1):
        strips(step)

    drain(NEAR, near)
    weigh([x for x in range(1, planes - 1) if x not in own[1:]])
    setup([x for x in range(planes) if x not in own])
    strips(ITERS - 1)
    for x in (0, 2, top - 1, top + 1):
        voxels([x, x + 1])

    drain(FAR, far)
    drain(SENT, sent)

    def place(value, x):
        return pltpu.roll(value, size_z - SLOT * x, 1)

    def weigh(xs):
        made = []
        for x in xs:
            w = ext[WEIGHT, x - 1] + ext[WEIGHT, x]
            w = w + down(w)
            value = speed(w + zdown(w), ext[PIN, x])
            low = pltpu.roll(srate[0], size_z - HALO - SLOT * x + size_z, 1)
            made.append((x, jnp.where(wide == 0, low, value)))
        for x, value in made:
            rate[x] = value

    loop(1, planes - 1, weigh, (planes - 2) // 2)

    def nodes(step, xs):
        made, masked = [], []
        last = step == ITERS - 1
        for x in xs:
            r = rate[x]
            if step == 0:
                r = jnp.where(ext[PIN, x] > 0.0, 0.0, r)
                masked.append((x, r))
            if last:
                r = jnp.where(wide == 0, pltpu.roll(srate[0], 2 * size_z - HALO - SLOT * x, 1), r)
            for c in range(3):
                minus, plus = node_sums(
                    [press[x - 1, 3 * c + k] for k in range(3)],
                    [press[x, 3 * c + k] for k in range(3)],
                    down,
                )
                plus = zdown(plus)
                beside = place(zin[step, c], x)
                if last:
                    minus = jnp.where(wide == size_z - 1, beside, minus)
                    plus = jnp.where(wide == 0, beside, plus)
                u = ext[c, x]
                fresh = advance(
                    u, lambda: prev[c, x], ext[INERT + c, x], r, minus + plus, omegas[step]
                )
                if not last:
                    fresh = jnp.where(edge, beside, fresh)
                made.append((x, c, u, fresh))
        if last:
            for x, c, _, fresh in made:
                out[c, x - HALO] = fresh[0:size_y]
            return
        later = [(x, c, make_terms(fresh)) for x, c, _, fresh in made]
        for x, r in masked:
            rate[x] = r
        for x, c, u, fresh in made:
            prev[c, x] = u
            ext[c, x] = fresh
        for x, c, three in later:
            for k in range(3):
                terms[x, 3 * c + k] = three[k]

    for step in range(ITERS):
        if step:
            all_voxels(step, planes - 1 - step)
        if step < ITERS - 1:
            loop(step + 1, planes - 1 - step, functools.partial(nodes, step), SLOT - 1 - step)

    loop(HALO, top, functools.partial(nodes, ITERS - 1), HALO)


def per_device(counts, start_disp, inertial, material, pinned, stiffness):
    size_x, size_y, size_z = material.shape
    planes, rows = size_x + 2 * HALO, 2 * size_y
    assert planes * SLOT == size_z and size_y == 2 * HALO and size_x == 2 * HALO
    hbm = pl.BlockSpec(memory_space=pl.ANY)
    f32 = lambda *shape: pltpu.VMEM(shape, jnp.float32)
    i32 = lambda *shape: pltpu.VMEM(shape, jnp.int32)
    return pl.pallas_call(
        functools.partial(kernel, counts),
        out_shape=pltpu.VMEM(start_disp.shape, jnp.float32),
        in_specs=[hbm] * 5,
        out_specs=pl.BlockSpec(memory_space=pltpu.VMEM),
        scratch_shapes=[
            pltpu.SMEM(stiffness.shape, jnp.float32),
            f32(3, size_x, size_y, size_z),
            i32(size_x, size_y, size_z),
            i32(size_x, size_y, size_z),
            f32(NARR, planes, rows, size_z),
            f32(4, size_y, size_z),
            f32(48, size_y, size_z),
            f32(2, NARR, rows, size_z),
            f32(2, 3, rows, size_z),
            f32(2, rows, size_z),
            f32(ITERS, 3, rows, size_z),
            f32(3, planes, rows, size_z),
            f32(planes, rows, size_z),
            f32(planes, 9, rows, size_z),
            f32(planes, 9, rows, size_z),
            f32(256, size_y, size_z),
            pltpu.SemaphoreType.DMA((FAR + 1,)),
            pltpu.SemaphoreType.DMA((2,)),
        ],
        compiler_params=pltpu.CompilerParams(collective_id=0, has_side_effects=True),
    )(start_disp, inertial, material, pinned, stiffness)


def solution(mesh):
    placed = (
        P(None, "gx", "gy", "gz"),
        P(None, "gx", "gy", "gz"),
        P("gx", "gy", "gz"),
        P("gx", "gy", "gz"),
        P(),
    )
    counts = tuple(mesh.shape[a] for a in AXES)
    return jax.shard_map(
        functools.partial(per_device, counts), mesh=mesh, in_specs=placed,
        out_specs=P(None, "gx", "gy", "gz"), check_vma=False,
    )
```

```python
import functools
import itertools

import jax
import jax.numpy as jnp
from jax import lax
from jax.experimental import pallas as pl
from jax.experimental.pallas import tpu as pltpu
from jax.sharding import PartitionSpec as P

ITERS = 4
POLAR_STEPS = 6
MATS = 8

relax = 0.6
radius = 0.9
HALO = ITERS
SLOT = 2 * HALO
NARR = 8
SPAN = NARR // 2
WEIGHT, INERT, PIN = 3, 4, 7
AXES = ("gx", "gy", "gz")
AROUND = tuple(
    o for n in (3, 2, 1) for o in itertools.product((-1, 0, 1), repeat=3) if sum(map(abs, o)) == n
)
DIAGONAL = tuple(itertools.product((-1, 1), repeat=2))
SENT, PIECES, HALVES, NEAR, FAR = 0, 1, 2, 4, 5


def loop(lo, hi, body, unroll=2):
    assert (hi - lo) % unroll == 0

    def group(k, _):
        body([lo + k * unroll + i for i in range(unroll)])
        return 0

    lax.fori_loop(0, (hi - lo) // unroll, group, 0)


def node_terms(u, uz, roll_y):
    zs, zd = uz + u, uz - u
    ys, yd = roll_y(zs), roll_y(zd)
    return zs + ys, ys - zs, zd + yd


def stretch(low, high):
    deform = []
    for c in range(3):
        dx = high[c][0] - low[c][0]
        dy = high[c][1] + low[c][1]
        dz = high[c][2] + low[c][2]
        row = [dx, dy, dz]
        row[c] = row[c] + 1.0
        deform.append(row)
    return deform


COSINE = (
    1.00000005, 1.15469445, -0.222086479, 0.105738212,
    -0.0606261262, 0.0323189784, -0.0123398994, 0.00230085802,
)


def stress(deform, w):
    f = deform
    s = {}
    for i in range(3):
        for j in range(i, 3):
            s[i, j] = f[0][i] * f[0][j] + f[1][i] * f[1][j] + f[2][i] * f[2][j]
    mean = (s[0, 0] + s[1, 1] + s[2, 2]) * (1.0 / 3.0)
    inv = jnp.minimum(lax.rsqrt(mean), 1.0)
    k11, k22, k33 = (s[i, i] - mean for i in range(3))
    k12, k13, k23 = s[0, 1], s[0, 2], s[1, 2]
    a11, a12, a13, a23 = k11 * k11, k12 * k12, k13 * k13, k23 * k23
    b11 = k22 * k33
    spread = jnp.maximum((a11 - b11 + a12 + (a13 + a23)) * (1.0 / 3.0), 1e-30)
    rp = lax.rsqrt(spread)
    rp2 = rp * rp
    b11 = b11 - a23
    b22 = k11 * k33 - a13
    b33 = k11 * k22 - a12
    b12 = k13 * k23 - k12 * k33
    b13 = k12 * k23 - k13 * k22
    b23 = k12 * k13 - k23 * k11
    det = k11 * b11 + (k12 * b12 + k13 * b13)
    half = 0.5 + 0.25 * (det * rp * rp2)
    half = jnp.maximum(half, 1e-12)
    root = half * lax.rsqrt(half)
    e = COSINE[-1]
    for a in COSINE[-2::-1]:
        e = e * root + a
    t2 = jnp.maximum(3.0 - 0.75 * (e * e), 1e-12)
    y = lax.rsqrt(t2)
    t = t2 * y
    e2 = 0.5 * e
    e3 = e + e2
    x2, x3 = t - e2, t + e2
    r12 = 1.0 / jnp.maximum(e3 - t, 1e-6)
    r13 = 1.0 / (e3 + t)
    r23 = 0.5 * y
    scale = 0.5 * (inv * inv)
    p = spread * rp * scale
    mean = mean * scale
    inv = inv * w
    qs = []
    for h in (mean + p * e, mean + p * x2, mean - p * x3):
        m = 1.5 - h
        q = inv * m
        for _ in range(POLAR_STEPS - 1):
            h = h * (m * m)
            m = 1.5 - h
            q = q * m
        qs.append(q)
    q12 = (qs[0] - qs[1]) * r12
    q23 = (qs[1] - qs[2]) * r23
    c2 = (q12 - q23) * r13
    c0 = ((w - qs[0]) - 3.0 * c2) + e * (q12 - c2 * x2)
    c1 = (c2 * x3 - q12) * rp
    c2 = c2 * rp2
    g = {
        (0, 0): (c0 + c1 * k11) - c2 * b11,
        (1, 1): (c0 + c1 * k22) - c2 * b22,
        (2, 2): (c0 + c1 * k33) - c2 * b33,
        (0, 1): c1 * k12 - c2 * b12,
        (0, 2): c1 * k13 - c2 * b13,
        (1, 2): c1 * k23 - c2 * b23,
    }
    pick = lambda i, j: g[min(i, j), max(i, j)]
    return [
        f[c][0] * pick(0, d) + f[c][1] * pick(1, d) + f[c][2] * pick(2, d)
        for c in range(3) for d in range(3)
    ]


def node_sums(before, here, roll_y):
    a = before[0] - here[0]
    b = before[1] + here[1]
    e = before[2] + here[2]
    g = (a - b) + roll_y(a + b)
    e = e + roll_y(e)
    return g - e, g + e


def advance(u, prev, inert, rate, f, omega):
    target = u - rate * ((u - inert) + f)
    return target if omega is None else omega * (target - prev()) + prev()


def kernel(
    counts, start, inertial, material, pinned, stiffness, out,
    stiff, first, mat, pins, ext, pk, rz, strip, sprev, srate, zin, prev, rate, terms, press,
    spare, copy_sem, load_sem,
):
    size_x, size_y, size_z = material.shape
    top = HALO + size_x
    planes = top + HALO
    rows = 2 * size_y
    own_y, own_x = pl.ds(0, size_y), pl.ds(HALO, size_x)
    here = [lax.axis_index(a) for a in AXES]
    has = [{-1: here[i] > 0, 1: here[i] < counts[i] - 1} for i in range(3)]

    loads = [
        pltpu.make_async_copy(pinned, pins, load_sem.at[0]),
        pltpu.make_async_copy(material, mat, load_sem.at[0]),
        pltpu.make_async_copy(inertial, ext.at[pl.ds(INERT, 3), own_x, own_y], load_sem.at[0]),
        pltpu.make_async_copy(start, first, load_sem.at[0]),
        pltpu.make_async_copy(stiffness, stiff, load_sem.at[1]),
    ]
    for copy in loads:
        copy.start()

    def exists(offset):
        found = None
        for i, o in enumerate(offset):
            if o:
                found = has[i][o] if found is None else found & has[i][o]
        return found

    def peer(offset):
        return {AXES[i]: here[i] + o for i, o in enumerate(offset) if o}

    blank = jnp.zeros((size_y, size_z), jnp.float32)

    def clear(xs, spots):
        for x in xs:
            for a in range(NARR):
                for spot in spots:
                    ext[a, x, spot * size_y : (spot + 1) * size_y] = blank

    def slot(z, spot, g, group):
        return 2 * (4 * (2 * z + spot) + g) + group

    for z in range(3):
        for spot in range(2):
            for g in range(4):
                if (z, spot) != (1, 0) or g in (0, 3):
                    for group in range(2):
                        rz[slot(z, spot, g, group)] = blank
    loop(0, HALO, lambda xs: clear(xs, (0, 1)), 2)
    loop(HALO, top, lambda xs: clear(xs, (1,)), 4)
    loop(top, planes, lambda xs: clear(xs, (0, 1)), 2)

    barrier = pltpu.get_barrier_semaphore()
    for offset in AROUND:
        @pl.when(exists(offset))
        def _(offset=offset):
            pl.semaphore_signal(
                barrier, inc=1, device_id=peer(offset), device_id_type=pl.DeviceIdType.MESH
            )

    sub = lax.broadcasted_iota(jnp.int32, (size_y, size_z), 0)
    lane = lax.broadcasted_iota(jnp.int32, (size_y, size_z), 1)
    inside = ((sub < size_y - 1) | has[1][1]) & ((lane < size_z - 1) | has[2][1])
    block = size_z // 4

    part = spare.at[pl.ds(0, 8 * size_x)]
    pltpu.make_async_copy(part, part, load_sem.at[0]).wait()
    loads[-1].wait()
    quarter = [stiff[i] * 0.25 for i in range(MATS)]

    for h in range(2):
        packed = [blank, blank]
        for i in range(HALO):
            x = HALO * h + i
            m = mat[x]
            w = jnp.zeros((size_y, size_z), jnp.float32)
            for index in range(MATS):
                w = jnp.where(m == index, quarter[index], w)
            keep = inside if x < size_x - 1 else inside & has[0][1]
            pin = pins[x] > 0
            inert = [ext[INERT + c, x + HALO, 0:size_y] for c in range(3)]
            arrays = [jnp.where(pin, inert[c], first[c, x]) for c in range(3)]
            arrays += [jnp.where(keep, w, 0.0)] + inert + [jnp.where(pin, 1.0, 0.0)]
            for a in (0, 1, 2, WEIGHT, PIN):
                ext[a, x + HALO, 0:size_y] = arrays[a]
            for a in range(NARR):
                spot = block * (a % SPAN) + SLOT * i
                moved = pltpu.roll(arrays[a], (spot + HALO) % size_z, 1)
                mine = (lane >= spot) & (lane < spot + SLOT)
                packed[a // SPAN] = jnp.where(mine, moved, packed[a // SPAN])
        for group in range(2):
            pk[2 * h + group] = packed[group]
            rz[slot(1, 0, 1 + h, group)] = packed[group]

    def remote(src, dst, k, offset):
        return pltpu.make_async_remote_copy(
            src_ref=src, dst_ref=dst, send_sem=copy_sem.at[SENT], recv_sem=copy_sem.at[k],
            device_id=peer(offset), device_id_type=pl.DeviceIdType.MESH,
        )

    def row_spans(dy, depth):
        if dy == 0:
            return own_y, own_y
        if dy > 0:
            return pl.ds(size_y - depth, depth), pl.ds(rows - depth, depth)
        return pl.ds(0, depth), pl.ds(size_y, depth)

    def plane_spans(dx, depth):
        if dx == 0:
            return own_x, own_x
        if dx > 0:
            return pl.ds(top - depth, depth), pl.ds(HALO - depth, depth)
        return pl.ds(HALO, depth), pl.ds(top, depth)

    def piece(offset):
        dx, dy, dz = offset
        h, g, n = {0: (0, 1, 2), 1: (1, 0, 1), -1: (0, 3, 1)}[dx]
        r, _ = row_spans(dy, HALO)
        to = slot(1 - dz, abs(dy), g, 0)
        return remote(pk.at[pl.ds(2 * h, 2 * n), r], rz.at[pl.ds(to, 2 * n), r], PIECES, offset)

    depths = (HALO, HALO - 1)
    sides = (-1, 1)

    def face(axis, side, group):
        offset = tuple(side if i == axis else 0 for i in range(3))
        x, x_to = plane_spans(offset[0], depths[group])
        y, y_to = row_spans(offset[1], depths[group])
        span = pl.ds(SPAN * group, SPAN)
        return remote(ext.at[span, x, y], ext.at[span, x_to, y_to], (NEAR, FAR)[group], offset)

    def half(side, part):
        x = pl.ds(HALO * (1 + part), HALO)
        y, y_to = row_spans(side, HALO)
        span = pl.ds(0, SPAN)
        return remote(ext.at[span, x, y], ext.at[span, x, y_to], HALVES + part, (0, side, 0))

    def corner(dx, dy, group):
        x, x_to = plane_spans(dx, depths[group])
        y, y_to = row_spans(dy, HALO)
        span = pl.ds(SPAN * group, SPAN)
        if group == 0:
            return remote(ext.at[span, x, y_to], ext.at[span, x_to, y_to], NEAR, (dx, 0, 0))
        return remote(ext.at[span, x, y], ext.at[span, x_to, y_to], FAR, (dx, dy, 0))

    def when(condition, action):
        pl.when(condition)(action)

    def send_face(axis, group):
        for side in sides:
            when(has[axis][side], lambda side=side: face(axis, side, group).start())

    near = lambda nx, ny, nz: 16 * nx + 8 * nx * ny
    far = lambda nx, ny, nz: 12 * nx + 12 * ny + 6 * nx * ny
    halves = lambda nx, ny, nz: 8 * ny
    pieces = lambda nx, ny, nz: (2 + nx) * (2 + ny) * (1 + nz) - 4

    def sent(*n):
        return pieces(*n) + 2 * halves(*n) + near(*n) + far(*n)

    beside = [has[i][-1].astype(jnp.int32) + has[i][1].astype(jnp.int32) for i in range(3)]
    choices = list(itertools.product(*[sorted({min(n - 1, 1), min(n - 1, 2)}) for n in counts]))

    def drain(k, tiles):
        for sizes in sorted({tiles(*n) for n in choices}):
            if not sizes:
                continue
            found = None
            for n in choices:
                if tiles(*n) == sizes:
                    same = (beside[0] == n[0]) & (beside[1] == n[1]) & (beside[2] == n[2])
                    found = same if found is None else found | same

            @pl.when(found)
            def _(sizes=sizes):
                part = spare.at[pl.ds(0, sizes)]
                pltpu.make_async_copy(part, part, copy_sem.at[k]).wait()

    pl.semaphore_wait(barrier, (1 + beside[0]) * (1 + beside[1]) * (1 + beside[2]) - 1)

    for part in range(2):
        for side in sides:
            when(has[1][side], lambda side=side, part=part: half(side, part).start())
    send_face(0, 0)
    for offset in AROUND:
        when(exists(offset), lambda offset=offset: piece(offset).start())
    send_face(1, 1)
    send_face(0, 1)

    for part, dx in enumerate(sides):
        drain(HALVES + part, halves)
        for dy in sides:
            when(has[0][dx] & has[1][-dy], lambda dx=dx, dy=dy: corner(dx, dy, 0).start())
    for dx, dy in DIAGONAL:
        when(exists((dx, dy)), lambda dx=dx, dy=dy: corner(dx, dy, 1).start())

    wide = lax.broadcasted_iota(jnp.int32, (rows, size_z), 1)
    edge = (wide == 0) | (wide == size_z - 1)
    up = lambda v: pltpu.roll(v, rows - 1, 0)
    down = lambda v: pltpu.roll(v, 1, 0)
    zup = lambda v: pltpu.roll(v, size_z - 1, 1)
    zdown = lambda v: pltpu.roll(v, 1, 1)
    xup = lambda v: pltpu.roll(v, size_z - SLOT, 1)
    xdown = lambda v: pltpu.roll(v, SLOT, 1)

    def make_terms(u):
        u = u * 0.25
        return node_terms(u, zup(u), up)

    def setup(xs):
        made = [(x, c, make_terms(ext[c, x])) for x in xs for c in range(3)]
        for x, c, three in made:
            for k in range(3):
                terms[x, 3 * c + k] = three[k]

    def voxels(xs):
        made = []
        for x in xs:
            low = [[terms[x, 3 * c + k] for k in range(3)] for c in range(3)]
            high = [[terms[x + 1, 3 * c + k] for k in range(3)] for c in range(3)]
            made.append((x, stress(stretch(low, high), ext[WEIGHT, x])))
        for x, p in made:
            for k in range(9):
                press[x, k] = p[k]

    def all_voxels(lo, hi):
        for x in range(hi - 1, lo - 1, -1):
            voxels([x])

    def weigh(xs):
        made = []
        for x in xs:
            w = ext[WEIGHT, x - 1] + ext[WEIGHT, x]
            w = w + down(w)
            made.append((x, relax / (1.0 + 0.75 * (w + zdown(w)))))
        for x, value in made:
            rate[x] = value

    own = list(range(HALO, top))
    weigh(own[1:])
    loop(HALO, top, setup, SLOT)
    all_voxels(HALO, top - 1)

    drain(PIECES, pieces)

    late = lax.rem(lane, SLOT) >= HALO
    for group in range(2):
        for s in range(2):
            for spot in range(2):
                parts = [
                    jnp.where(
                        late, rz[slot(s + 1, spot, g, group)], rz[slot(s, spot, g, group)]
                    )
                    for g in range(4)
                ]
                for j in range(SPAN):
                    value = None
                    for g in range(4):
                        moved = parts[g]
                        if g != j:
                            moved = pltpu.roll(moved, (block * (g - j)) % size_z, 1)
                        value = moved if g == 0 else jnp.where(lane >= block * g, moved, value)
                    strip[s, SPAN * group + j, size_y * spot : size_y * (spot + 1)] = value

    def speed(total, pin):
        return jnp.where(pin > 0.0, 0.0, relax / (1.0 + 0.75 * total))

    for s in range(2):
        w = strip[s, WEIGHT]
        w = w + xdown(w)
        w = w + down(w)
        srate[s] = speed(w + zdown(w), strip[s, PIN])

    joint = lax.rem(wide, SLOT) == HALO

    def bring(low, high):
        return pltpu.roll(jnp.where(joint, low, high), size_z - HALO, 1)

    omegas = [None, 2.0 / (2.0 - radius * radius)]
    while len(omegas) < ITERS:
        omegas.append(4.0 / (4.0 - radius * radius * omegas[-1]))

    def strips(step):
        made = []
        for s in range(2):
            low, high = [], []
            for c in range(3):
                u = strip[s, c] * 0.25
                low.append(node_terms(u, zup(u), up))
                high.append(node_terms(xup(u), pltpu.roll(u, size_z - SLOT - 1, 1), up))
            made.append(stress(stretch(low, high), strip[s, WEIGHT]))
        for c in range(3):
            fresh = []
            for s in range(2):
                a, b, e = made[s][3 * c : 3 * c + 3]
                both, less = a + b, a - b
                e = e + down(e)
                here, before = down(-less) - both, less + down(both)
                last = step == ITERS - 1
                if not last:
                    u = strip[s, c]
                    f = (here - e) + xdown(before - e)
                    f = f + (zdown(here + e) + pltpu.roll(before + e, SLOT + 1, 1))
                    fresh.append(advance(
                        u, lambda: sprev[s, c], strip[s, INERT + c], srate[s], f, omegas[step]
                    ))
                    sprev[s, c] = u
                    strip[s, c] = fresh[s]
                elif s == 0:
                    fresh.append(zdown(here + e) + pltpu.roll(before + e, SLOT + 1, 1))
                else:
                    fresh.append((here - e) + xdown(before - e))
            zin[step, c] = bring(*fresh)

    for step in range(ITERS - 1):
        strips(step)

    drain(NEAR, near)
    weigh([x for x in range(1, planes - 1) if x not in own[1:]])
    setup([x for x in range(planes) if x not in own])
    strips(ITERS - 1)
    for x in (0, 2, top - 1, top + 1):
        voxels([x, x + 1])

    drain(FAR, far)
    drain(SENT, sent)

    def place(value, x):
        return pltpu.roll(value, size_z - SLOT * x, 1)

    def nodes(step, xs):
        made, masked = [], []
        last = step == ITERS - 1
        for x in xs:
            r = rate[x]
            if step == 0:
                r = jnp.where(ext[PIN, x] > 0.0, 0.0, r)
                masked.append((x, r))
            if last:
                r = jnp.where(wide == 0, pltpu.roll(srate[0], 2 * size_z - HALO - SLOT * x, 1), r)
            for c in range(3):
                minus, plus = node_sums(
                    [press[x - 1, 3 * c + k] for k in range(3)],
                    [press[x, 3 * c + k] for k in range(3)],
                    down,
                )
                plus = zdown(plus)
                beside = place(zin[step, c], x)
                if last:
                    minus = jnp.where(wide == size_z - 1, beside, minus)
                    plus = jnp.where(wide == 0, beside, plus)
                u = ext[c, x]
                fresh = advance(
                    u, lambda: prev[c, x], ext[INERT + c, x], r, minus + plus, omegas[step]
                )
                if not last:
                    fresh = jnp.where(edge, beside, fresh)
                made.append((x, c, u, fresh))
        if last:
            for x, c, _, fresh in made:
                out[c, x - HALO] = fresh[0:size_y]
            return
        later = [(x, c, make_terms(fresh)) for x, c, _, fresh in made]
        for x, r in masked:
            rate[x] = r
        for x, c, u, fresh in made:
            prev[c, x] = u
            ext[c, x] = fresh
        for x, c, three in later:
            for k in range(3):
                terms[x, 3 * c + k] = three[k]

    for step in range(ITERS):
        if step:
            all_voxels(step, planes - 1 - step)
        if step < ITERS - 1:
            nodes(step, list(range(planes - 2 - step, step, -1)))

    nodes(ITERS - 1, list(range(HALO, top)))


def per_device(counts, start_disp, inertial, material, pinned, stiffness):
    size_x, size_y, size_z = material.shape
    planes, rows = size_x + 2 * HALO, 2 * size_y
    assert planes * SLOT == size_z and size_y == 2 * HALO and size_x == 2 * HALO
    hbm = pl.BlockSpec(memory_space=pl.ANY)
    f32 = lambda *shape: pltpu.VMEM(shape, jnp.float32)
    i32 = lambda *shape: pltpu.VMEM(shape, jnp.int32)
    return pl.pallas_call(
        functools.partial(kernel, counts),
        out_shape=pltpu.VMEM(start_disp.shape, jnp.float32),
        in_specs=[hbm] * 5,
        out_specs=pl.BlockSpec(memory_space=pltpu.VMEM),
        scratch_shapes=[
            pltpu.SMEM(stiffness.shape, jnp.float32),
            f32(3, size_x, size_y, size_z),
            i32(size_x, size_y, size_z),
            i32(size_x, size_y, size_z),
            f32(NARR, planes, rows, size_z),
            f32(4, size_y, size_z),
            f32(48, size_y, size_z),
            f32(2, NARR, rows, size_z),
            f32(2, 3, rows, size_z),
            f32(2, rows, size_z),
            f32(ITERS, 3, rows, size_z),
            f32(3, planes, rows, size_z),
            f32(planes, rows, size_z),
            f32(planes, 9, rows, size_z),
            f32(planes, 9, rows, size_z),
            f32(256, size_y, size_z),
            pltpu.SemaphoreType.DMA((FAR + 1,)),
            pltpu.SemaphoreType.DMA((2,)),
        ],
        compiler_params=pltpu.CompilerParams(collective_id=0, has_side_effects=True),
    )(start_disp, inertial, material, pinned, stiffness)


def solution(mesh):
    placed = (
        P(None, "gx", "gy", "gz"),
        P(None, "gx", "gy", "gz"),
        P("gx", "gy", "gz"),
        P("gx", "gy", "gz"),
        P(),
    )
    counts = tuple(mesh.shape[a] for a in AXES)
    return jax.shard_map(
        functools.partial(per_device, counts), mesh=mesh, in_specs=placed,
        out_specs=P(None, "gx", "gy", "gz"), check_vma=False,
    )
```

```python
import functools
import itertools

import jax
import jax.numpy as jnp
from jax import lax
from jax.experimental import pallas as pl
from jax.experimental.pallas import tpu as pltpu
from jax.sharding import PartitionSpec as P

ITERS = 4
POLAR_STEPS = 6
MATS = 8

relax = 0.6
radius = 0.9
HALO = ITERS
SLOT = 2 * HALO
NARR = 8
SPAN = NARR // 2
WEIGHT, INERT, PIN = 3, 4, 7
AXES = ("gx", "gy", "gz")
AROUND = tuple(
    o for n in (3, 2, 1) for o in itertools.product((-1, 0, 1), repeat=3) if sum(map(abs, o)) == n
)
DIAGONAL = tuple(itertools.product((-1, 1), repeat=2))
SENT, PIECES, HALVES, NEAR, FAR = 0, 1, 2, 4, 5


def loop(lo, hi, body, unroll=2):
    assert (hi - lo) % unroll == 0

    def group(k, _):
        body([lo + k * unroll + i for i in range(unroll)])
        return 0

    lax.fori_loop(0, (hi - lo) // unroll, group, 0)


def node_terms(u, uz, roll_y):
    zs, zd = uz + u, uz - u
    ys, yd = roll_y(zs), roll_y(zd)
    return zs + ys, ys - zs, zd + yd


def stretch(low, high):
    deform = []
    for c in range(3):
        dx = high[c][0] - low[c][0]
        dy = high[c][1] + low[c][1]
        dz = high[c][2] + low[c][2]
        row = [dx, dy, dz]
        row[c] = row[c] + 1.0
        deform.append(row)
    return deform


COSINE = (
    1.00000005, 1.15469445, -0.222086479, 0.105738212,
    -0.0606261262, 0.0323189784, -0.0123398994, 0.00230085802,
)


def stress(deform, w):
    f = deform
    s = {}
    for i in range(3):
        for j in range(i, 3):
            s[i, j] = f[0][i] * f[0][j] + f[1][i] * f[1][j] + f[2][i] * f[2][j]
    mean = (s[0, 0] + s[1, 1] + s[2, 2]) * (1.0 / 3.0)
    inv = jnp.minimum(lax.rsqrt(mean), 1.0)
    k11, k22, k33 = (s[i, i] - mean for i in range(3))
    k12, k13, k23 = s[0, 1], s[0, 2], s[1, 2]
    a11, a12, a13, a23 = k11 * k11, k12 * k12, k13 * k13, k23 * k23
    b11 = k22 * k33
    spread = jnp.maximum((a11 - b11 + a12 + (a13 + a23)) * (1.0 / 3.0), 1e-30)
    rp = lax.rsqrt(spread)
    rp2 = rp * rp
    b11 = b11 - a23
    b22 = k11 * k33 - a13
    b33 = k11 * k22 - a12
    b12 = k13 * k23 - k12 * k33
    b13 = k12 * k23 - k13 * k22
    b23 = k12 * k13 - k23 * k11
    det = k11 * b11 + (k12 * b12 + k13 * b13)
    half = 0.5 + 0.25 * (det * rp * rp2)
    half = jnp.maximum(half, 1e-12)
    root = half * lax.rsqrt(half)
    e = COSINE[-1]
    for a in COSINE[-2::-1]:
        e = e * root + a
    t2 = jnp.maximum(3.0 - 0.75 * (e * e), 1e-12)
    y = lax.rsqrt(t2)
    t = t2 * y
    e2 = 0.5 * e
    e3 = e + e2
    x2, x3 = t - e2, t + e2
    r12 = 1.0 / jnp.maximum(e3 - t, 1e-6)
    r13 = 1.0 / (e3 + t)
    r23 = 0.5 * y
    scale = 0.5 * (inv * inv)
    p = spread * rp * scale
    mean = mean * scale
    inv = inv * w
    qs = []
    for h in (mean + p * e, mean + p * x2, mean - p * x3):
        m = 1.5 - h
        q = inv * m
        for _ in range(POLAR_STEPS - 1):
            h = h * (m * m)
            m = 1.5 - h
            q = q * m
        qs.append(q)
    q12 = (qs[0] - qs[1]) * r12
    q23 = (qs[1] - qs[2]) * r23
    c2 = (q12 - q23) * r13
    c0 = ((w - qs[0]) - 3.0 * c2) + e * (q12 - c2 * x2)
    c1 = (c2 * x3 - q12) * rp
    c2 = c2 * rp2
    g = {
        (0, 0): (c0 + c1 * k11) - c2 * b11,
        (1, 1): (c0 + c1 * k22) - c2 * b22,
        (2, 2): (c0 + c1 * k33) - c2 * b33,
        (0, 1): c1 * k12 - c2 * b12,
        (0, 2): c1 * k13 - c2 * b13,
        (1, 2): c1 * k23 - c2 * b23,
    }
    pick = lambda i, j: g[min(i, j), max(i, j)]
    return [
        f[c][0] * pick(0, d) + f[c][1] * pick(1, d) + f[c][2] * pick(2, d)
        for c in range(3) for d in range(3)
    ]


def node_sums(before, here, roll_y):
    a = before[0] - here[0]
    b = before[1] + here[1]
    e = before[2] + here[2]
    g = (a - b) + roll_y(a + b)
    e = e + roll_y(e)
    return g - e, g + e


def advance(u, prev, inert, rate, f, omega):
    target = u - rate * ((u - inert) + f)
    return target if omega is None else omega * (target - prev()) + prev()


def kernel(
    counts, start, inertial, material, pinned, stiffness, out,
    stiff, first, mat, pins, ext, pk, rz, strip, sprev, srate, zin, prev, rate, terms, press, edge_w,
    spare, copy_sem, load_sem,
):
    size_x, size_y, size_z = material.shape
    top = HALO + size_x
    planes = top + HALO
    rows = 2 * size_y
    own_y, own_x = pl.ds(0, size_y), pl.ds(HALO, size_x)
    here = [lax.axis_index(a) for a in AXES]
    has = [{-1: here[i] > 0, 1: here[i] < counts[i] - 1} for i in range(3)]

    loads = [
        pltpu.make_async_copy(pinned, pins, load_sem.at[0]),
        pltpu.make_async_copy(material, mat, load_sem.at[0]),
        pltpu.make_async_copy(inertial, ext.at[pl.ds(INERT, 3), own_x, own_y], load_sem.at[0]),
        pltpu.make_async_copy(start, first, load_sem.at[0]),
        pltpu.make_async_copy(stiffness, stiff, load_sem.at[1]),
    ]
    for copy in loads:
        copy.start()

    def exists(offset):
        found = None
        for i, o in enumerate(offset):
            if o:
                found = has[i][o] if found is None else found & has[i][o]
        return found

    def peer(offset):
        return {AXES[i]: here[i] + o for i, o in enumerate(offset) if o}

    blank = jnp.zeros((size_y, size_z), jnp.float32)

    def clear(xs, spots):
        for x in xs:
            for a in range(NARR):
                for spot in spots:
                    ext[a, x, spot * size_y : (spot + 1) * size_y] = blank

    def slot(z, spot, g, group):
        return 2 * (4 * (2 * z + spot) + g) + group

    for z in range(3):
        for spot in range(2):
            for g in range(4):
                if (z, spot) != (1, 0) or g in (0, 3):
                    for group in range(2):
                        rz[slot(z, spot, g, group)] = blank
    loop(0, HALO, lambda xs: clear(xs, (0, 1)), 2)
    loop(HALO, top, lambda xs: clear(xs, (1,)), 4)
    loop(top, planes, lambda xs: clear(xs, (0, 1)), 2)

    barrier = pltpu.get_barrier_semaphore()
    for offset in AROUND:
        @pl.when(exists(offset))
        def _(offset=offset):
            pl.semaphore_signal(
                barrier, inc=1, device_id=peer(offset), device_id_type=pl.DeviceIdType.MESH
            )

    sub = lax.broadcasted_iota(jnp.int32, (size_y, size_z), 0)
    lane = lax.broadcasted_iota(jnp.int32, (size_y, size_z), 1)
    inside = ((sub < size_y - 1) | has[1][1]) & ((lane < size_z - 1) | has[2][1])
    block = size_z // 4

    part = spare.at[pl.ds(0, 8 * size_x)]
    pltpu.make_async_copy(part, part, load_sem.at[0]).wait()
    loads[-1].wait()
    quarter = [stiff[i] * 0.25 for i in range(MATS)]

    for h in range(2):
        packed = [blank, blank]
        for i in range(HALO):
            x = HALO * h + i
            m = mat[x]
            w = jnp.zeros((size_y, size_z), jnp.float32)
            for index in range(MATS):
                w = jnp.where(m == index, quarter[index], w)
            keep = inside if x < size_x - 1 else inside & has[0][1]
            pin = pins[x] > 0
            inert = [ext[INERT + c, x + HALO, 0:size_y] for c in range(3)]
            arrays = [jnp.where(pin, inert[c], first[c, x]) for c in range(3)]
            arrays += [jnp.where(keep, w, 0.0)] + inert + [jnp.where(pin, 1.0, 0.0)]
            for a in (0, 1, 2, WEIGHT, PIN):
                ext[a, x + HALO, 0:size_y] = arrays[a]
            for a in range(NARR):
                spot = block * (a % SPAN) + SLOT * i
                moved = pltpu.roll(arrays[a], (spot + HALO) % size_z, 1)
                mine = (lane >= spot) & (lane < spot + SLOT)
                packed[a // SPAN] = jnp.where(mine, moved, packed[a // SPAN])
        for group in range(2):
            pk[2 * h + group] = packed[group]
            rz[slot(1, 0, 1 + h, group)] = packed[group]

    def remote(src, dst, k, offset):
        return pltpu.make_async_remote_copy(
            src_ref=src, dst_ref=dst, send_sem=copy_sem.at[SENT], recv_sem=copy_sem.at[k],
            device_id=peer(offset), device_id_type=pl.DeviceIdType.MESH,
        )

    def row_spans(dy, depth):
        if dy == 0:
            return own_y, own_y
        if dy > 0:
            return pl.ds(size_y - depth, depth), pl.ds(rows - depth, depth)
        return pl.ds(0, depth), pl.ds(size_y, depth)

    def plane_spans(dx, depth):
        if dx == 0:
            return own_x, own_x
        if dx > 0:
            return pl.ds(top - depth, depth), pl.ds(HALO - depth, depth)
        return pl.ds(HALO, depth), pl.ds(top, depth)

    def piece(offset):
        dx, dy, dz = offset
        h, g, n = {0: (0, 1, 2), 1: (1, 0, 1), -1: (0, 3, 1)}[dx]
        r, _ = row_spans(dy, HALO)
        to = slot(1 - dz, abs(dy), g, 0)
        return remote(pk.at[pl.ds(2 * h, 2 * n), r], rz.at[pl.ds(to, 2 * n), r], PIECES, offset)

    depths = (HALO, HALO - 1)
    sides = (-1, 1)

    def face(axis, side, group):
        offset = tuple(side if i == axis else 0 for i in range(3))
        x, x_to = plane_spans(offset[0], depths[group])
        y, y_to = row_spans(offset[1], depths[group])
        span = pl.ds(SPAN * group, SPAN)
        return remote(ext.at[span, x, y], ext.at[span, x_to, y_to], (NEAR, FAR)[group], offset)

    def half(side, part):
        x = pl.ds(HALO * (1 + part), HALO)
        y, y_to = row_spans(side, HALO)
        span = pl.ds(0, SPAN)
        return remote(ext.at[span, x, y], ext.at[span, x, y_to], HALVES + part, (0, side, 0))

    def corner(dx, dy, group):
        x, x_to = plane_spans(dx, depths[group])
        y, y_to = row_spans(dy, HALO)
        span = pl.ds(SPAN * group, SPAN)
        if group == 0:
            return remote(ext.at[span, x, y_to], ext.at[span, x_to, y_to], NEAR, (dx, 0, 0))
        return remote(ext.at[span, x, y], ext.at[span, x_to, y_to], FAR, (dx, dy, 0))

    def when(condition, action):
        pl.when(condition)(action)

    def send_face(axis, group):
        for side in sides:
            when(has[axis][side], lambda side=side: face(axis, side, group).start())

    near = lambda nx, ny, nz: 16 * nx + 8 * nx * ny
    far = lambda nx, ny, nz: 12 * nx + 12 * ny + 6 * nx * ny
    halves = lambda nx, ny, nz: 8 * ny
    pieces = lambda nx, ny, nz: (2 + nx) * (2 + ny) * (1 + nz) - 4

    def sent(*n):
        return pieces(*n) + 2 * halves(*n) + near(*n) + far(*n)

    beside = [has[i][-1].astype(jnp.int32) + has[i][1].astype(jnp.int32) for i in range(3)]
    choices = list(itertools.product(*[sorted({min(n - 1, 1), min(n - 1, 2)}) for n in counts]))

    def drain(k, tiles):
        for sizes in sorted({tiles(*n) for n in choices}):
            if not sizes:
                continue
            found = None
            for n in choices:
                if tiles(*n) == sizes:
                    same = (beside[0] == n[0]) & (beside[1] == n[1]) & (beside[2] == n[2])
                    found = same if found is None else found | same

            @pl.when(found)
            def _(sizes=sizes):
                part = spare.at[pl.ds(0, sizes)]
                pltpu.make_async_copy(part, part, copy_sem.at[k]).wait()

    pl.semaphore_wait(barrier, (1 + beside[0]) * (1 + beside[1]) * (1 + beside[2]) - 1)

    for part in range(2):
        for side in sides:
            when(has[1][side], lambda side=side, part=part: half(side, part).start())
    send_face(0, 0)
    for offset in AROUND:
        when(exists(offset), lambda offset=offset: piece(offset).start())
    send_face(1, 1)
    send_face(0, 1)

    for part, dx in enumerate(sides):
        drain(HALVES + part, halves)
        for dy in sides:
            when(has[0][dx] & has[1][-dy], lambda dx=dx, dy=dy: corner(dx, dy, 0).start())
    for dx, dy in DIAGONAL:
        when(exists((dx, dy)), lambda dx=dx, dy=dy: corner(dx, dy, 1).start())

    wide = lax.broadcasted_iota(jnp.int32, (rows, size_z), 1)
    edge = (wide == 0) | (wide == size_z - 1)
    up = lambda v: pltpu.roll(v, rows - 1, 0)
    down = lambda v: pltpu.roll(v, 1, 0)
    zup = lambda v: pltpu.roll(v, size_z - 1, 1)
    zdown = lambda v: pltpu.roll(v, 1, 1)
    xup = lambda v: pltpu.roll(v, size_z - SLOT, 1)
    xdown = lambda v: pltpu.roll(v, SLOT, 1)

    def make_terms(u):
        u = u * 0.25
        return node_terms(u, zup(u), up)

    def line(x, k, n=rows):
        return pl.ds((9 * x + k) * rows, n)

    def setup(xs):
        made = [(x, c, make_terms(ext[c, x])) for x in xs for c in range(3)]
        for x, c, three in made:
            for k in range(3):
                terms[line(x, 3 * c + k)] = three[k]

    def voxels(xs, n=rows):
        for x in xs:
            low = [[terms[line(x, 3 * c + k, n)] for k in range(3)] for c in range(3)]
            high = [[terms[line(x + 1, 3 * c + k, n)] for k in range(3)] for c in range(3)]
            p = stress(stretch(low, high), ext[WEIGHT, x, 0:n])
            for k in range(9):
                press[line(x, k, n)] = p[k]

    def last_voxels():
        lo = ITERS - 1

        def across(x, k):
            return pl.ds((9 * x + k + 1) * rows - 1, size_y, 9 * rows)

        voxels([top - 1])
        low = [[terms[across(lo, 3 * c + k)] for k in range(3)] for c in range(3)]
        high = [[terms[across(lo + 1, 3 * c + k)] for k in range(3)] for c in range(3)]
        p = stress(stretch(low, high), edge_w[...])
        for k in range(9):
            press[across(lo, k)] = p[k]
        for x in range(top - 2, lo - 1, -1):
            voxels([x], size_y)

    def all_voxels(lo, hi):
        for x in range(hi - 1, lo - 1, -1):
            voxels([x])

    def weigh(xs):
        made = []
        for x in xs:
            w = ext[WEIGHT, x - 1] + ext[WEIGHT, x]
            w = w + down(w)
            made.append((x, relax / (1.0 + 0.75 * (w + zdown(w)))))
        for x, value in made:
            rate[x] = value

    own = list(range(HALO, top))
    weigh(own[1:])
    setup(own)
    all_voxels(HALO, top - 1)

    drain(PIECES, pieces)

    late = lax.rem(lane, SLOT) >= HALO
    for group in range(2):
        for s in range(2):
            for spot in range(2):
                parts = [
                    jnp.where(
                        late, rz[slot(s + 1, spot, g, group)], rz[slot(s, spot, g, group)]
                    )
                    for g in range(4)
                ]
                for j in range(SPAN):
                    value = None
                    for g in range(4):
                        moved = parts[g]
                        if g != j:
                            moved = pltpu.roll(moved, (block * (g - j)) % size_z, 1)
                        value = moved if g == 0 else jnp.where(lane >= block * g, moved, value)
                    strip[s, SPAN * group + j, size_y * spot : size_y * (spot + 1)] = value

    def speed(total, pin):
        return jnp.where(pin > 0.0, 0.0, relax / (1.0 + 0.75 * total))

    for s in range(2):
        w = strip[s, WEIGHT]
        w = w + xdown(w)
        w = w + down(w)
        srate[s] = speed(w + zdown(w), strip[s, PIN])

    joint = lax.rem(wide, SLOT) == HALO

    def bring(low, high):
        return pltpu.roll(jnp.where(joint, low, high), size_z - HALO, 1)

    omegas = [None, 2.0 / (2.0 - radius * radius)]
    while len(omegas) < ITERS:
        omegas.append(4.0 / (4.0 - radius * radius * omegas[-1]))

    def strips(step):
        made = []
        for s in range(2):
            low, high = [], []
            for c in range(3):
                u = strip[s, c] * 0.25
                low.append(node_terms(u, zup(u), up))
                high.append(node_terms(xup(u), pltpu.roll(u, size_z - SLOT - 1, 1), up))
            made.append(stress(stretch(low, high), strip[s, WEIGHT]))
        for c in range(3):
            fresh = []
            for s in range(2):
                a, b, e = made[s][3 * c : 3 * c + 3]
                both, less = a + b, a - b
                e = e + down(e)
                here, before = down(-less) - both, less + down(both)
                last = step == ITERS - 1
                if not last:
                    u = strip[s, c]
                    f = (here - e) + xdown(before - e)
                    f = f + (zdown(here + e) + pltpu.roll(before + e, SLOT + 1, 1))
                    fresh.append(advance(
                        u, lambda: sprev[s, c], strip[s, INERT + c], srate[s], f, omegas[step]
                    ))
                    sprev[s, c] = u
                    strip[s, c] = fresh[s]
                elif s == 0:
                    fresh.append(zdown(here + e) + pltpu.roll(before + e, SLOT + 1, 1))
                else:
                    fresh.append((here - e) + xdown(before - e))
            zin[step, c] = bring(*fresh)

    for step in range(ITERS - 1):
        strips(step)

    drain(NEAR, near)
    for i in range(size_y):
        edge_w[i : i + 1] = ext[WEIGHT, ITERS - 1 + i, rows - 1 : rows]
    weigh([x for x in range(1, planes - 1) if x not in own[1:]])
    setup([x for x in range(planes) if x not in own])
    strips(ITERS - 1)
    for x in (0, 2, top - 1, top + 1):
        voxels([x, x + 1])

    drain(FAR, far)
    drain(SENT, sent)

    def place(value, x):
        return pltpu.roll(value, size_z - SLOT * x, 1)

    def nodes(step, xs):
        made, masked = [], []
        last = step == ITERS - 1
        for x in xs:
            r = rate[x]
            if step == 0:
                r = jnp.where(ext[PIN, x] > 0.0, 0.0, r)
                masked.append((x, r))
            if last:
                r = jnp.where(wide == 0, pltpu.roll(srate[0], 2 * size_z - HALO - SLOT * x, 1), r)
            for c in range(3):
                minus, plus = node_sums(
                    [press[line(x - 1, 3 * c + k)] for k in range(3)],
                    [press[line(x, 3 * c + k)] for k in range(3)],
                    down,
                )
                plus = zdown(plus)
                beside = place(zin[step, c], x)
                if last:
                    minus = jnp.where(wide == size_z - 1, beside, minus)
                    plus = jnp.where(wide == 0, beside, plus)
                u = ext[c, x]
                fresh = advance(
                    u, lambda: prev[c, x], ext[INERT + c, x], r, minus + plus, omegas[step]
                )
                if not last:
                    fresh = jnp.where(edge, beside, fresh)
                made.append((x, c, u, fresh))
        if last:
            for x, c, _, fresh in made:
                out[c, x - HALO] = fresh[0:size_y]
            return
        later = [(x, c, make_terms(fresh)) for x, c, _, fresh in made]
        for x, r in masked:
            rate[x] = r
        for x, c, u, fresh in made:
            prev[c, x] = u
            ext[c, x] = fresh
        for x, c, three in later:
            for k in range(3):
                terms[line(x, 3 * c + k)] = three[k]

    for step in range(ITERS):
        if step == ITERS - 1:
            last_voxels()
        elif step:
            all_voxels(step, planes - 1 - step)
        if step < ITERS - 1:
            nodes(step, list(range(planes - 2 - step, step, -1)))

    nodes(ITERS - 1, list(range(HALO, top)))


def per_device(counts, start_disp, inertial, material, pinned, stiffness):
    size_x, size_y, size_z = material.shape
    planes, rows = size_x + 2 * HALO, 2 * size_y
    assert planes * SLOT == size_z and size_y == 2 * HALO and size_x == 2 * HALO
    hbm = pl.BlockSpec(memory_space=pl.ANY)
    f32 = lambda *shape: pltpu.VMEM(shape, jnp.float32)
    i32 = lambda *shape: pltpu.VMEM(shape, jnp.int32)
    return pl.pallas_call(
        functools.partial(kernel, counts),
        out_shape=pltpu.VMEM(start_disp.shape, jnp.float32),
        in_specs=[hbm] * 5,
        out_specs=pl.BlockSpec(memory_space=pltpu.VMEM),
        scratch_shapes=[
            pltpu.SMEM(stiffness.shape, jnp.float32),
            f32(3, size_x, size_y, size_z),
            i32(size_x, size_y, size_z),
            i32(size_x, size_y, size_z),
            f32(NARR, planes, rows, size_z),
            f32(4, size_y, size_z),
            f32(48, size_y, size_z),
            f32(2, NARR, rows, size_z),
            f32(2, 3, rows, size_z),
            f32(2, rows, size_z),
            f32(ITERS, 3, rows, size_z),
            f32(3, planes, rows, size_z),
            f32(planes, rows, size_z),
            f32(planes * 9 * rows, size_z),
            f32(planes * 9 * rows, size_z),
            f32(size_y, size_z),
            f32(256, size_y, size_z),
            pltpu.SemaphoreType.DMA((FAR + 1,)),
            pltpu.SemaphoreType.DMA((2,)),
        ],
        compiler_params=pltpu.CompilerParams(collective_id=0, has_side_effects=True),
    )(start_disp, inertial, material, pinned, stiffness)


def solution(mesh):
    placed = (
        P(None, "gx", "gy", "gz"),
        P(None, "gx", "gy", "gz"),
        P("gx", "gy", "gz"),
        P("gx", "gy", "gz"),
        P(),
    )
    counts = tuple(mesh.shape[a] for a in AXES)
    return jax.shard_map(
        functools.partial(per_device, counts), mesh=mesh, in_specs=placed,
        out_specs=P(None, "gx", "gy", "gz"), check_vma=False,
    )
```

```python
import functools
import itertools

import jax
import jax.numpy as jnp
from jax import lax
from jax.experimental import pallas as pl
from jax.experimental.pallas import tpu as pltpu
from jax.sharding import PartitionSpec as P

ITERS = 4
POLAR_STEPS = 6
MATS = 8

relax = 0.6
radius = 0.9
HALO = ITERS
SLOT = 2 * HALO
NARR = 8
SPAN = NARR // 2
WEIGHT, INERT, PIN = 3, 4, 7
FOLDED = ITERS - 3
AXES = ("gx", "gy", "gz")
AROUND = tuple(
    o for n in (3, 2, 1) for o in itertools.product((-1, 0, 1), repeat=3) if sum(map(abs, o)) == n
)
DIAGONAL = tuple(itertools.product((-1, 1), repeat=2))
SENT, PIECES, HALVES, NEAR, FAR = 0, 1, 2, 4, 5


def loop(lo, hi, body, unroll=2):
    assert (hi - lo) % unroll == 0

    def group(k, _):
        body([lo + k * unroll + i for i in range(unroll)])
        return 0

    lax.fori_loop(0, (hi - lo) // unroll, group, 0)


def node_terms(u, uz, roll_y):
    zs, zd = uz + u, uz - u
    ys, yd = roll_y(zs), roll_y(zd)
    return zs + ys, ys - zs, zd + yd


def stretch(low, high):
    deform = []
    for c in range(3):
        dx = high[c][0] - low[c][0]
        dy = high[c][1] + low[c][1]
        dz = high[c][2] + low[c][2]
        row = [dx, dy, dz]
        row[c] = row[c] + 1.0
        deform.append(row)
    return deform


COSINE = (
    1.00000005, 1.15469445, -0.222086479, 0.105738212,
    -0.0606261262, 0.0323189784, -0.0123398994, 0.00230085802,
)


def stress(deform, w):
    f = deform
    s = {}
    for i in range(3):
        for j in range(i, 3):
            s[i, j] = f[0][i] * f[0][j] + f[1][i] * f[1][j] + f[2][i] * f[2][j]
    mean = (s[0, 0] + s[1, 1] + s[2, 2]) * (1.0 / 3.0)
    inv = jnp.minimum(lax.rsqrt(mean), 1.0)
    k11, k22, k33 = (s[i, i] - mean for i in range(3))
    k12, k13, k23 = s[0, 1], s[0, 2], s[1, 2]
    a11, a12, a13, a23 = k11 * k11, k12 * k12, k13 * k13, k23 * k23
    b11 = k22 * k33
    spread = jnp.maximum((a11 - b11 + a12 + (a13 + a23)) * (1.0 / 3.0), 1e-30)
    rp = lax.rsqrt(spread)
    rp2 = rp * rp
    b11 = b11 - a23
    b22 = k11 * k33 - a13
    b33 = k11 * k22 - a12
    b12 = k13 * k23 - k12 * k33
    b13 = k12 * k23 - k13 * k22
    b23 = k12 * k13 - k23 * k11
    det = k11 * b11 + (k12 * b12 + k13 * b13)
    half = 0.5 + 0.25 * (det * rp * rp2)
    half = jnp.maximum(half, 1e-12)
    root = half * lax.rsqrt(half)
    e = COSINE[-1]
    for a in COSINE[-2::-1]:
        e = e * root + a
    t2 = jnp.maximum(3.0 - 0.75 * (e * e), 1e-12)
    y = lax.rsqrt(t2)
    t = t2 * y
    e2 = 0.5 * e
    e3 = e + e2
    x2, x3 = t - e2, t + e2
    r12 = 1.0 / jnp.maximum(e3 - t, 1e-6)
    r13 = 1.0 / (e3 + t)
    r23 = 0.5 * y
    scale = 0.5 * (inv * inv)
    p = spread * rp * scale
    mean = mean * scale
    inv = inv * w
    qs = []
    for h in (mean + p * e, mean + p * x2, mean - p * x3):
        m = 1.5 - h
        q = inv * m
        for _ in range(POLAR_STEPS - 1):
            h = h * (m * m)
            m = 1.5 - h
            q = q * m
        qs.append(q)
    q12 = (qs[0] - qs[1]) * r12
    q23 = (qs[1] - qs[2]) * r23
    c2 = (q12 - q23) * r13
    c0 = ((w - qs[0]) - 3.0 * c2) + e * (q12 - c2 * x2)
    c1 = (c2 * x3 - q12) * rp
    c2 = c2 * rp2
    g = {
        (0, 0): (c0 + c1 * k11) - c2 * b11,
        (1, 1): (c0 + c1 * k22) - c2 * b22,
        (2, 2): (c0 + c1 * k33) - c2 * b33,
        (0, 1): c1 * k12 - c2 * b12,
        (0, 2): c1 * k13 - c2 * b13,
        (1, 2): c1 * k23 - c2 * b23,
    }
    pick = lambda i, j: g[min(i, j), max(i, j)]
    return [
        f[c][0] * pick(0, d) + f[c][1] * pick(1, d) + f[c][2] * pick(2, d)
        for c in range(3) for d in range(3)
    ]


def node_sums(before, here, roll_y):
    a = before[0] - here[0]
    b = before[1] + here[1]
    e = before[2] + here[2]
    g = (a - b) + roll_y(a + b)
    e = e + roll_y(e)
    return g - e, g + e


def advance(u, prev, inert, rate, f, omega):
    target = u - rate * ((u - inert) + f)
    return target if omega is None else omega * (target - prev()) + prev()


def kernel(
    counts, start, inertial, material, pinned, stiffness, out,
    stiff, first, mat, pins, ext, pk, rz, strip, sprev, srate, zin, prev, rate, terms, press, edge_w,
    spare, copy_sem, load_sem,
):
    size_x, size_y, size_z = material.shape
    top = HALO + size_x
    planes = top + HALO
    rows = 2 * size_y
    own_y, own_x = pl.ds(0, size_y), pl.ds(HALO, size_x)
    here = [lax.axis_index(a) for a in AXES]
    has = [{-1: here[i] > 0, 1: here[i] < counts[i] - 1} for i in range(3)]

    loads = [
        pltpu.make_async_copy(pinned, pins, load_sem.at[0]),
        pltpu.make_async_copy(material, mat, load_sem.at[0]),
        pltpu.make_async_copy(inertial, ext.at[pl.ds(INERT, 3), own_x, own_y], load_sem.at[0]),
        pltpu.make_async_copy(start, first, load_sem.at[0]),
        pltpu.make_async_copy(stiffness, stiff, load_sem.at[1]),
    ]
    for copy in loads:
        copy.start()

    def exists(offset):
        found = None
        for i, o in enumerate(offset):
            if o:
                found = has[i][o] if found is None else found & has[i][o]
        return found

    def peer(offset):
        return {AXES[i]: here[i] + o for i, o in enumerate(offset) if o}

    blank = jnp.zeros((size_y, size_z), jnp.float32)

    def clear(xs, spots):
        for x in xs:
            for a in range(NARR):
                for spot in spots:
                    ext[a, x, spot * size_y : (spot + 1) * size_y] = blank

    def slot(z, spot, g, group):
        return 2 * (4 * (2 * z + spot) + g) + group

    for z in range(3):
        for spot in range(2):
            for g in range(4):
                if (z, spot) != (1, 0) or g in (0, 3):
                    for group in range(2):
                        rz[slot(z, spot, g, group)] = blank
    loop(0, HALO, lambda xs: clear(xs, (0, 1)), 2)
    loop(HALO, top, lambda xs: clear(xs, (1,)), 4)
    loop(top, planes, lambda xs: clear(xs, (0, 1)), 2)

    barrier = pltpu.get_barrier_semaphore()
    for offset in AROUND:
        @pl.when(exists(offset))
        def _(offset=offset):
            pl.semaphore_signal(
                barrier, inc=1, device_id=peer(offset), device_id_type=pl.DeviceIdType.MESH
            )

    sub = lax.broadcasted_iota(jnp.int32, (size_y, size_z), 0)
    lane = lax.broadcasted_iota(jnp.int32, (size_y, size_z), 1)
    inside = ((sub < size_y - 1) | has[1][1]) & ((lane < size_z - 1) | has[2][1])
    block = size_z // 4

    part = spare.at[pl.ds(0, 8 * size_x)]
    pltpu.make_async_copy(part, part, load_sem.at[0]).wait()
    loads[-1].wait()
    quarter = [stiff[i] * 0.25 for i in range(MATS)]

    for h in range(2):
        packed = [blank, blank]
        for i in range(HALO):
            x = HALO * h + i
            m = mat[x]
            w = jnp.zeros((size_y, size_z), jnp.float32)
            for index in range(MATS):
                w = jnp.where(m == index, quarter[index], w)
            keep = inside if x < size_x - 1 else inside & has[0][1]
            pin = pins[x] > 0
            inert = [ext[INERT + c, x + HALO, 0:size_y] for c in range(3)]
            arrays = [jnp.where(pin, inert[c], first[c, x]) for c in range(3)]
            arrays += [jnp.where(keep, w, 0.0)] + inert + [jnp.where(pin, 1.0, 0.0)]
            for a in (0, 1, 2, WEIGHT, PIN):
                ext[a, x + HALO, 0:size_y] = arrays[a]
            for a in range(NARR):
                spot = block * (a % SPAN) + SLOT * i
                moved = pltpu.roll(arrays[a], (spot + HALO) % size_z, 1)
                mine = (lane >= spot) & (lane < spot + SLOT)
                packed[a // SPAN] = jnp.where(mine, moved, packed[a // SPAN])
        for group in range(2):
            pk[2 * h + group] = packed[group]
            rz[slot(1, 0, 1 + h, group)] = packed[group]

    def remote(src, dst, k, offset):
        return pltpu.make_async_remote_copy(
            src_ref=src, dst_ref=dst, send_sem=copy_sem.at[SENT], recv_sem=copy_sem.at[k],
            device_id=peer(offset), device_id_type=pl.DeviceIdType.MESH,
        )

    def row_spans(dy, depth):
        if dy == 0:
            return own_y, own_y
        if dy > 0:
            return pl.ds(size_y - depth, depth), pl.ds(rows - depth, depth)
        return pl.ds(0, depth), pl.ds(size_y, depth)

    def plane_spans(dx, depth):
        if dx == 0:
            return own_x, own_x
        if dx > 0:
            return pl.ds(top - depth, depth), pl.ds(HALO - depth, depth)
        return pl.ds(HALO, depth), pl.ds(top, depth)

    def piece(offset):
        dx, dy, dz = offset
        h, g, n = {0: (0, 1, 2), 1: (1, 0, 1), -1: (0, 3, 1)}[dx]
        r, _ = row_spans(dy, HALO)
        to = slot(1 - dz, abs(dy), g, 0)
        return remote(pk.at[pl.ds(2 * h, 2 * n), r], rz.at[pl.ds(to, 2 * n), r], PIECES, offset)

    depths = (HALO, HALO - 1)
    sides = (-1, 1)

    def face(axis, side, group):
        offset = tuple(side if i == axis else 0 for i in range(3))
        x, x_to = plane_spans(offset[0], depths[group])
        y, y_to = row_spans(offset[1], depths[group])
        span = pl.ds(SPAN * group, SPAN)
        return remote(ext.at[span, x, y], ext.at[span, x_to, y_to], (NEAR, FAR)[group], offset)

    def half(side, part):
        x = pl.ds(HALO * (1 + part), HALO)
        y, y_to = row_spans(side, HALO)
        span = pl.ds(0, SPAN)
        return remote(ext.at[span, x, y], ext.at[span, x, y_to], HALVES + part, (0, side, 0))

    def corner(dx, dy, group):
        x, x_to = plane_spans(dx, depths[group])
        y, y_to = row_spans(dy, HALO)
        span = pl.ds(SPAN * group, SPAN)
        if group == 0:
            return remote(ext.at[span, x, y_to], ext.at[span, x_to, y_to], NEAR, (dx, 0, 0))
        return remote(ext.at[span, x, y], ext.at[span, x_to, y_to], FAR, (dx, dy, 0))

    def when(condition, action):
        pl.when(condition)(action)

    def send_face(axis, group):
        for side in sides:
            when(has[axis][side], lambda side=side: face(axis, side, group).start())

    near = lambda nx, ny, nz: 16 * nx + 8 * nx * ny
    far = lambda nx, ny, nz: 12 * nx + 12 * ny + 6 * nx * ny
    halves = lambda nx, ny, nz: 8 * ny
    pieces = lambda nx, ny, nz: (2 + nx) * (2 + ny) * (1 + nz) - 4

    def sent(*n):
        return pieces(*n) + 2 * halves(*n) + near(*n) + far(*n)

    beside = [has[i][-1].astype(jnp.int32) + has[i][1].astype(jnp.int32) for i in range(3)]
    choices = list(itertools.product(*[sorted({min(n - 1, 1), min(n - 1, 2)}) for n in counts]))

    def drain(k, tiles):
        for sizes in sorted({tiles(*n) for n in choices}):
            if not sizes:
                continue
            found = None
            for n in choices:
                if tiles(*n) == sizes:
                    same = (beside[0] == n[0]) & (beside[1] == n[1]) & (beside[2] == n[2])
                    found = same if found is None else found | same

            @pl.when(found)
            def _(sizes=sizes):
                part = spare.at[pl.ds(0, sizes)]
                pltpu.make_async_copy(part, part, copy_sem.at[k]).wait()

    pl.semaphore_wait(barrier, (1 + beside[0]) * (1 + beside[1]) * (1 + beside[2]) - 1)

    for part in range(2):
        for side in sides:
            when(has[1][side], lambda side=side, part=part: half(side, part).start())
    send_face(0, 0)
    for offset in AROUND:
        when(exists(offset), lambda offset=offset: piece(offset).start())
    send_face(1, 1)
    send_face(0, 1)

    for part, dx in enumerate(sides):
        drain(HALVES + part, halves)
        for dy in sides:
            when(has[0][dx] & has[1][-dy], lambda dx=dx, dy=dy: corner(dx, dy, 0).start())
    for dx, dy in DIAGONAL:
        when(exists((dx, dy)), lambda dx=dx, dy=dy: corner(dx, dy, 1).start())

    wide = lax.broadcasted_iota(jnp.int32, (rows, size_z), 1)
    edge = (wide == 0) | (wide == size_z - 1)
    up = lambda v: pltpu.roll(v, rows - 1, 0)
    down = lambda v: pltpu.roll(v, 1, 0)
    zup = lambda v: pltpu.roll(v, size_z - 1, 1)
    zdown = lambda v: pltpu.roll(v, 1, 1)
    xup = lambda v: pltpu.roll(v, size_z - SLOT, 1)
    xdown = lambda v: pltpu.roll(v, SLOT, 1)

    def make_terms(u):
        u = u * 0.25
        return node_terms(u, zup(u), up)

    def line(x, k, n=rows):
        return pl.ds((9 * x + k) * rows, n)

    def setup(xs):
        made = [(x, c, make_terms(ext[c, x])) for x in xs for c in range(3)]
        for x, c, three in made:
            for k in range(3):
                terms[line(x, 3 * c + k)] = three[k]

    def voxels(xs, n=rows):
        for x in xs:
            low = [[terms[line(x, 3 * c + k, n)] for k in range(3)] for c in range(3)]
            high = [[terms[line(x + 1, 3 * c + k, n)] for k in range(3)] for c in range(3)]
            p = stress(stretch(low, high), ext[WEIGHT, x, 0:n])
            for k in range(9):
                press[line(x, k, n)] = p[k]

    def rim(step):
        depth = ITERS - 1 - step
        return [*range(rows - depth - 1, rows), *range(size_y, size_y + depth)]

    rims = [(step, row) for step in range(FOLDED, ITERS) for row in rim(step)]

    def folded_voxels(step):
        def across(x, k, row):
            return pl.ds((9 * x + k) * rows + row, size_y, 9 * rows)

        for x in range(planes - 2 - step, step + size_y - 1, -1):
            voxels([x])
        for row in rim(step):
            low = [[terms[across(step, 3 * c + k, row)] for k in range(3)] for c in range(3)]
            high = [[terms[across(step + 1, 3 * c + k, row)] for k in range(3)] for c in range(3)]
            p = stress(stretch(low, high), edge_w[rims.index((step, row))])
            for k in range(9):
                press[across(step, k, row)] = p[k]
        for x in range(step + size_y - 1, step - 1, -1):
            voxels([x], size_y)

    def all_voxels(lo, hi):
        for x in range(hi - 1, lo - 1, -1):
            voxels([x])

    def weigh(xs):
        made = []
        for x in xs:
            w = ext[WEIGHT, x - 1] + ext[WEIGHT, x]
            w = w + down(w)
            made.append((x, relax / (1.0 + 0.75 * (w + zdown(w)))))
        for x, value in made:
            rate[x] = value

    own = list(range(HALO, top))
    weigh(own[1:])
    setup(own)
    all_voxels(HALO, top - 1)

    drain(PIECES, pieces)

    late = lax.rem(lane, SLOT) >= HALO
    for group in range(2):
        for s in range(2):
            for spot in range(2):
                parts = [
                    jnp.where(
                        late, rz[slot(s + 1, spot, g, group)], rz[slot(s, spot, g, group)]
                    )
                    for g in range(4)
                ]
                for j in range(SPAN):
                    value = None
                    for g in range(4):
                        moved = parts[g]
                        if g != j:
                            moved = pltpu.roll(moved, (block * (g - j)) % size_z, 1)
                        value = moved if g == 0 else jnp.where(lane >= block * g, moved, value)
                    strip[s, SPAN * group + j, size_y * spot : size_y * (spot + 1)] = value

    def speed(total, pin):
        return jnp.where(pin > 0.0, 0.0, relax / (1.0 + 0.75 * total))

    for s in range(2):
        w = strip[s, WEIGHT]
        w = w + xdown(w)
        w = w + down(w)
        srate[s] = speed(w + zdown(w), strip[s, PIN])

    joint = lax.rem(wide, SLOT) == HALO

    def bring(low, high):
        return pltpu.roll(jnp.where(joint, low, high), size_z - HALO, 1)

    omegas = [None, 2.0 / (2.0 - radius * radius)]
    while len(omegas) < ITERS:
        omegas.append(4.0 / (4.0 - radius * radius * omegas[-1]))

    def strips(step):
        made = []
        for s in range(2):
            low, high = [], []
            for c in range(3):
                u = strip[s, c] * 0.25
                low.append(node_terms(u, zup(u), up))
                high.append(node_terms(xup(u), pltpu.roll(u, size_z - SLOT - 1, 1), up))
            made.append(stress(stretch(low, high), strip[s, WEIGHT]))
        for c in range(3):
            fresh = []
            for s in range(2):
                a, b, e = made[s][3 * c : 3 * c + 3]
                both, less = a + b, a - b
                e = e + down(e)
                here, before = down(-less) - both, less + down(both)
                last = step == ITERS - 1
                if not last:
                    u = strip[s, c]
                    f = (here - e) + xdown(before - e)
                    f = f + (zdown(here + e) + pltpu.roll(before + e, SLOT + 1, 1))
                    fresh.append(advance(
                        u, lambda: sprev[s, c], strip[s, INERT + c], srate[s], f, omegas[step]
                    ))
                    sprev[s, c] = u
                    strip[s, c] = fresh[s]
                elif s == 0:
                    fresh.append(zdown(here + e) + pltpu.roll(before + e, SLOT + 1, 1))
                else:
                    fresh.append((here - e) + xdown(before - e))
            zin[step, c] = bring(*fresh)

    for step in range(ITERS - 1):
        strips(step)

    drain(NEAR, near)
    for k, (step, row) in enumerate(rims):
        for i in range(size_y):
            edge_w[k, i : i + 1] = ext[WEIGHT, step + i, row : row + 1]
    weigh([x for x in range(1, planes - 1) if x not in own[1:]])
    setup([x for x in range(planes) if x not in own])
    strips(ITERS - 1)
    for x in (0, 2, top - 1, top + 1):
        voxels([x, x + 1])

    drain(FAR, far)
    drain(SENT, sent)

    def place(value, x):
        return pltpu.roll(value, size_z - SLOT * x, 1)

    def nodes(step, xs):
        made, masked = [], []
        last = step == ITERS - 1
        for x in xs:
            r = rate[x]
            if step == 0:
                r = jnp.where(ext[PIN, x] > 0.0, 0.0, r)
                masked.append((x, r))
            if last:
                r = jnp.where(wide == 0, pltpu.roll(srate[0], 2 * size_z - HALO - SLOT * x, 1), r)
            for c in range(3):
                minus, plus = node_sums(
                    [press[line(x - 1, 3 * c + k)] for k in range(3)],
                    [press[line(x, 3 * c + k)] for k in range(3)],
                    down,
                )
                plus = zdown(plus)
                beside = place(zin[step, c], x)
                if last:
                    minus = jnp.where(wide == size_z - 1, beside, minus)
                    plus = jnp.where(wide == 0, beside, plus)
                u = ext[c, x]
                fresh = advance(
                    u, lambda: prev[c, x], ext[INERT + c, x], r, minus + plus, omegas[step]
                )
                if not last:
                    fresh = jnp.where(edge, beside, fresh)
                made.append((x, c, u, fresh))
        if last:
            for x, c, _, fresh in made:
                out[c, x - HALO] = fresh[0:size_y]
            return
        later = [(x, c, make_terms(fresh)) for x, c, _, fresh in made]
        for x, r in masked:
            rate[x] = r
        for x, c, u, fresh in made:
            prev[c, x] = u
            ext[c, x] = fresh
        for x, c, three in later:
            for k in range(3):
                terms[line(x, 3 * c + k)] = three[k]

    for step in range(ITERS):
        if step >= FOLDED:
            folded_voxels(step)
        elif step:
            all_voxels(step, planes - 1 - step)
        if step < ITERS - 1:
            nodes(step, list(range(planes - 2 - step, step, -1)))

    nodes(ITERS - 1, list(range(HALO, top)))


def per_device(counts, start_disp, inertial, material, pinned, stiffness):
    size_x, size_y, size_z = material.shape
    planes, rows = size_x + 2 * HALO, 2 * size_y
    assert planes * SLOT == size_z and size_y == 2 * HALO and size_x == 2 * HALO
    hbm = pl.BlockSpec(memory_space=pl.ANY)
    f32 = lambda *shape: pltpu.VMEM(shape, jnp.float32)
    i32 = lambda *shape: pltpu.VMEM(shape, jnp.int32)
    return pl.pallas_call(
        functools.partial(kernel, counts),
        out_shape=pltpu.VMEM(start_disp.shape, jnp.float32),
        in_specs=[hbm] * 5,
        out_specs=pl.BlockSpec(memory_space=pltpu.VMEM),
        scratch_shapes=[
            pltpu.SMEM(stiffness.shape, jnp.float32),
            f32(3, size_x, size_y, size_z),
            i32(size_x, size_y, size_z),
            i32(size_x, size_y, size_z),
            f32(NARR, planes, rows, size_z),
            f32(4, size_y, size_z),
            f32(48, size_y, size_z),
            f32(2, NARR, rows, size_z),
            f32(2, 3, rows, size_z),
            f32(2, rows, size_z),
            f32(ITERS, 3, rows, size_z),
            f32(3, planes, rows, size_z),
            f32(planes, rows, size_z),
            f32(planes * 9 * rows, size_z),
            f32(planes * 9 * rows, size_z),
            f32(SLOT * ITERS, size_y, size_z),
            f32(256, size_y, size_z),
            pltpu.SemaphoreType.DMA((FAR + 1,)),
            pltpu.SemaphoreType.DMA((2,)),
        ],
        compiler_params=pltpu.CompilerParams(collective_id=0, has_side_effects=True),
    )(start_disp, inertial, material, pinned, stiffness)


def solution(mesh):
    placed = (
        P(None, "gx", "gy", "gz"),
        P(None, "gx", "gy", "gz"),
        P("gx", "gy", "gz"),
        P("gx", "gy", "gz"),
        P(),
    )
    counts = tuple(mesh.shape[a] for a in AXES)
    return jax.shard_map(
        functools.partial(per_device, counts), mesh=mesh, in_specs=placed,
        out_specs=P(None, "gx", "gy", "gz"), check_vma=False,
    )
```
